32 devices in a mesh: dp: 2 (over x), tp: 4 (over z), sp: 4 (over y, core).
Axes of the slice: x: 2, y: 2, z: 4, core: 2. Of those that a mesh axis runs over, the one named last changes fastest.
Arguments:
- tok_hidden: bfloat16 [512, 4096], P('dp'), parts along dimension 0
- cache_len: int32 [512], P('dp'), parts along dimension 0
- k_cache: bfloat16 [512, 32, 64, 128], P('dp', 'tp', 'sp'), parts along dimension 0
- v_cache: bfloat16 [512, 32, 64, 128], P('dp', 'tp', 'sp'), parts along dimension 0
- ln_gain: float32 [4096], replicated
- ln_bias: float32 [4096], replicated
- w_qkv: bfloat16 [4096, 3, 32, 128], P(None, None, 'tp')
- b_qkv: bfloat16 [3, 32, 128], P(None, 'tp')
- w_out: bfloat16 [32, 128, 4096], P('tp')
- b_out: bfloat16 [4096], replicated
Outputs:
- output 1: bfloat16 [512, 4096], P('dp'), parts along dimension 0
- output 2: bfloat16 [512, 32, 64, 128], P('dp', 'tp', 'sp'), parts along dimension 0
- output 3: bfloat16 [512, 32, 64, 128], P('dp', 'tp', 'sp'), parts along dimension 0
There are 2 independent parts. The reference program is written for one: setup_inputs(seed, part) draws one part's arguments, and reference() takes and returns one part's arrays. A program takes and returns all parts, laid end to end along the dimension named above; an argument that names none is the same for every part.
All inputs are finite; a program needn't handle non-finite values.
Results may differ from the reference program's by a relative error of at most 0.00849222.
Values sent between devices are 32-bit elements.
A program may use at most 1 GiB of HBM per device.

```python
import jax
import jax.numpy as jnp
from jax import lax

BATCH_ROWS = 256
MODEL_DIM = 4096
NUM_HEADS = 32
HEAD_DIM = 128
MAX_LEN = 64


def setup_inputs(seed: int = 0, part: int = 0) -> dict:
    shared_key, part_root = jax.random.split(jax.random.key(seed))
    part_key = jax.random.fold_in(part_root, part)
    part_keys = jax.random.split(part_key, 5)
    shared_keys = jax.random.split(shared_key, 6)
    cache_shape = (BATCH_ROWS, NUM_HEADS, MAX_LEN, HEAD_DIM)
    tok_hidden = 0.5 * jax.random.normal(part_keys[0], (BATCH_ROWS, MODEL_DIM), jnp.float32)
    cache_len = jax.random.randint(part_keys[1], (BATCH_ROWS,), 0, MAX_LEN, jnp.int32)
    cache_len = cache_len.at[0].set(MAX_LEN - 1).at[1].set(0)
    k_cache = 2.0 * jax.random.normal(part_keys[2], cache_shape, jnp.float32)
    coarse = jax.random.normal(part_keys[3], (BATCH_ROWS, NUM_HEADS, 16, HEAD_DIM), jnp.float32)
    v_cache = jnp.repeat(coarse, MAX_LEN // 16, axis=2) + 0.7 * jax.random.normal(part_keys[4], cache_shape, jnp.float32)
    ln_gain = 1.0 + 0.2 * jax.random.normal(shared_keys[0], (MODEL_DIM,), jnp.float32)
    ln_bias = 0.2 * jax.random.normal(shared_keys[1], (MODEL_DIM,), jnp.float32)
    w_qkv = jax.random.normal(shared_keys[2], (MODEL_DIM, 3, NUM_HEADS, HEAD_DIM), jnp.float32) * MODEL_DIM ** -0.5
    b_qkv = 0.3 * jax.random.normal(shared_keys[3], (3, NUM_HEADS, HEAD_DIM), jnp.float32)
    w_out = jax.random.normal(shared_keys[4], (NUM_HEADS, HEAD_DIM, MODEL_DIM), jnp.float32) * (NUM_HEADS * HEAD_DIM) ** -0.5
    b_out = 0.3 * jax.random.normal(shared_keys[5], (MODEL_DIM,), jnp.float32)
    return {
        'tok_hidden': tok_hidden.astype(jnp.bfloat16),
        'cache_len': cache_len,
        'k_cache': k_cache.astype(jnp.bfloat16),
        'v_cache': v_cache.astype(jnp.bfloat16),
        'ln_gain': ln_gain,
        'ln_bias': ln_bias,
        'w_qkv': w_qkv.astype(jnp.bfloat16),
        'b_qkv': b_qkv.astype(jnp.bfloat16),
        'w_out': w_out.astype(jnp.bfloat16),
        'b_out': b_out.astype(jnp.bfloat16),
    }


def reference(tok_hidden, cache_len, k_cache, v_cache, ln_gain, ln_bias, w_qkv, b_qkv, w_out, b_out):
    x_f32 = tok_hidden.astype(jnp.float32)
    mean_x = jnp.mean(x_f32, axis=-1, keepdims=True)
    centered = x_f32 - mean_x
    var_x = jnp.mean(centered * centered, axis=-1, keepdims=True)
    hidden = (centered * lax.rsqrt(var_x + 1e-5) * ln_gain + ln_bias).astype(jnp.bfloat16)
    qkv_flat = jnp.dot(hidden, w_qkv.reshape(MODEL_DIM, 3 * NUM_HEADS * HEAD_DIM), preferred_element_type=jnp.float32)
    qkv_all = (qkv_flat + b_qkv.reshape(3 * NUM_HEADS * HEAD_DIM).astype(jnp.float32)).astype(jnp.bfloat16)
    qkv_all = qkv_all.reshape(BATCH_ROWS, 3, NUM_HEADS, HEAD_DIM)
    q_new = qkv_all[:, 0]
    k_new = qkv_all[:, 1]
    v_new = qkv_all[:, 2]
    slots = jnp.arange(MAX_LEN, dtype=jnp.int32)
    write_mask = (slots[None, :] == cache_len[:, None])[:, None, :, None]
    k_out = jnp.where(write_mask, k_new[:, :, None, :], k_cache)
    v_out = jnp.where(write_mask, v_new[:, :, None, :], v_cache)

    def one_row(row_args):
        q_row, k_row, v_row, row_len = row_args
        scores = jnp.einsum('hd,hsd->hs', q_row.astype(jnp.float32), k_row.astype(jnp.float32)) * HEAD_DIM ** -0.5
        valid = slots[None, :] <= row_len
        prob_w = jax.nn.softmax(jnp.where(valid, scores, -jnp.inf), axis=-1)
        prob_w = prob_w.astype(jnp.bfloat16).astype(jnp.float32)
        return jnp.einsum('hs,hsd->hd', prob_w, v_row.astype(jnp.float32))

    attended = lax.map(one_row, (q_new, k_out, v_out, cache_len))
    projected = jnp.dot(attended.astype(jnp.bfloat16).reshape(BATCH_ROWS, NUM_HEADS * HEAD_DIM), w_out.reshape(NUM_HEADS * HEAD_DIM, MODEL_DIM), preferred_element_type=jnp.float32)
    y_out = (x_f32 + projected + b_out.astype(jnp.float32)).astype(jnp.bfloat16)
    return y_out, k_out, v_out
```

```python
import functools

import jax
import jax.numpy as jnp
from jax import lax
from jax.experimental import pallas as pl
from jax.experimental.pallas import tpu as pltpu
from jax.sharding import PartitionSpec as P

MESH = pl.DeviceIdType.MESH
NEG = -1e30
F32 = jnp.float32
BF16 = jnp.bfloat16


def norm_project(tok_hidden, ln_gain, ln_bias, w_qkv, b_qkv):
    x_f32 = tok_hidden.astype(F32)
    mean_x = jnp.mean(x_f32, axis=-1, keepdims=True)
    centered = x_f32 - mean_x
    var_x = jnp.mean(centered * centered, axis=-1, keepdims=True)
    hidden = (centered * lax.rsqrt(var_x + 1e-5) * ln_gain + ln_bias).astype(BF16)
    qkv_all = jnp.einsum('bm,mthd->thbd', hidden, w_qkv, preferred_element_type=F32)
    return (qkv_all + b_qkv.astype(F32)[:, :, None, :]).astype(BF16)


def attend_kernel(slots, per_stat, len_ref, qkv_ref, k_ref, v_ref, ko_ref, vo_ref, acc_ref, st_ref, qkv_f32):
    rows, heads, _, dim = k_ref.shape
    step = pl.program_id(0)
    first = lax.axis_index('sp') * slots
    qkv_f32[...] = qkv_ref[...].astype(F32)
    slot = lax.broadcasted_iota(jnp.int32, (slots, dim), 0)
    flat = heads * slots
    row_id = lax.broadcasted_iota(jnp.int32, (heads, flat), 0)
    col_id = lax.broadcasted_iota(jnp.int32, (heads, flat), 1)
    in_head = (col_id // slots) == row_id
    col_slot = jnp.where(in_head, col_id % slots, slots)
    lane = lax.broadcasted_iota(jnp.int32, (heads, 128), 1)
    group = lax.rem(step, per_stat // rows)

    @pl.when(group == 0)
    def _():
        st_ref[...] = jnp.zeros_like(st_ref)

    stat = st_ref[0]
    for b in range(rows):
        local = len_ref[step * rows + b] - first
        hit = (slot == local)[None]
        k_new = jnp.broadcast_to(qkv_f32[1, :, b:b + 1, :], (heads, slots, dim)).astype(BF16)
        v_new = jnp.broadcast_to(qkv_f32[2, :, b:b + 1, :], (heads, slots, dim)).astype(BF16)
        k_all = jnp.where(hit, k_new, k_ref[b])
        v_all = jnp.where(hit, v_new, v_ref[b])
        ko_ref[b] = k_all
        vo_ref[b] = v_all
        q = qkv_f32[0, :, b, :].astype(BF16)
        s = lax.dot_general(q, k_all.reshape(flat, dim), (((1,), (1,)), ((), ())), preferred_element_type=F32)
        valid = col_slot <= jnp.minimum(local, slots - 1)
        s = jnp.where(valid, s * dim ** -0.5, NEG)
        top = jnp.max(s, axis=1, keepdims=True)
        w = jnp.where(valid, jnp.exp(s - top), 0.0)
        total = jnp.sum(w, axis=1, keepdims=True)
        acc_ref[b] = jnp.dot(w.astype(BF16), v_all.reshape(flat, dim), preferred_element_type=F32)
        at = group * rows + b
        stat = jnp.where(lane == at, top, stat)
        stat = jnp.where(lane == per_stat + at, total, stat)
    st_ref[0] = stat


def attend(qkv, cache_len, k_cache, v_cache, block, per_stat):
    rows, heads, slots, dim = k_cache.shape
    cache_block = pl.BlockSpec((block, heads, slots, dim), lambda i: (i, 0, 0, 0))
    return pl.pallas_call(
        functools.partial(attend_kernel, slots, per_stat),
        grid=(rows // block,),
        in_specs=[
            pl.BlockSpec(memory_space=pltpu.SMEM),
            pl.BlockSpec((3, heads, block, dim), lambda i: (0, 0, i, 0)),
            cache_block,
            cache_block,
        ],
        out_specs=[
            cache_block,
            cache_block,
            pl.BlockSpec((block, heads, dim), lambda i: (i, 0, 0)),
            pl.BlockSpec((1, heads, 128), lambda i: (i * block // per_stat, 0, 0)),
        ],
        out_shape=[
            jax.ShapeDtypeStruct(k_cache.shape, BF16),
            jax.ShapeDtypeStruct(v_cache.shape, BF16),
            jax.ShapeDtypeStruct((rows, heads, dim), F32),
            jax.ShapeDtypeStruct((rows // per_stat, heads, 128), F32),
        ],
        scratch_shapes=[pltpu.VMEM((3, heads, block, dim), F32)],
        compiler_params=pltpu.CompilerParams(dimension_semantics=("arbitrary",)),
    )(cache_len, qkv, k_cache, v_cache)


def combine_kernel(quarter, rc, cc, acc_ref, st_ref, x_hbm, w_hbm, b_ref, y_ref,
                   got_acc, got_st, fwd_acc, fwd_st, own_acc, far_acc, far_st, att,
                   w_buf, x_buf, mine, near, half, far_half, tot, from_y, from_c, from_yc, load_sem,
                   a_s, a_r, as_s, as_r, b_s, b_r, bs_s, bs_r,
                   x_s, x_r, p_s, p_r, t_s, t_r, y_s, y_r, c_s, c_r, f_s, f_r):
    heads, dim = acc_ref.shape[1:]
    n_row, n_col = quarter // rc, w_hbm.shape[1] // cc
    n = n_row * n_col
    r = lax.axis_index('sp')
    z = lax.axis_index('tp')
    core, chip_y = lax.rem(r, 2), r // 2
    mate = {'sp': chip_y * 2 + (1 - core)}
    across = {'sp': (1 - chip_y) * 2 + core}
    outer = (z == 0) | (z == 3)
    inward = {'tp': jnp.where(z == 0, 1, 2)}
    outward = {'tp': jnp.where(z == 1, 0, 3)}
    peer = {'tp': 3 - z}

    load_x = pltpu.make_async_copy(x_hbm, x_buf, load_sem.at[0])
    load_x.start()
    w_loads = []
    for j in range(n_col):
        cp = pltpu.make_async_copy(w_hbm.at[:, pl.ds(j * cc, cc)], w_buf.at[:, pl.ds(j * cc, cc)], load_sem.at[1 + j])
        cp.start()
        w_loads.append(cp)

    barrier = pltpu.get_barrier_semaphore()
    pl.semaphore_signal(barrier, inc=1, device_id=mate, device_id_type=MESH)
    pl.semaphore_signal(barrier, inc=1, device_id=across, device_id_type=MESH)

    @pl.when(outer)
    def _():
        pl.semaphore_signal(barrier, inc=1, device_id=inward, device_id_type=MESH)
        pl.semaphore_wait(barrier, 3)

    @pl.when(jnp.logical_not(outer))
    def _():
        pl.semaphore_signal(barrier, inc=1, device_id=outward, device_id_type=MESH)
        pl.semaphore_signal(barrier, inc=1, device_id=peer, device_id_type=MESH)
        pl.semaphore_wait(barrier, 4)

    def remote(src, dst, s, rcv, dev):
        return pltpu.make_async_remote_copy(src_ref=src, dst_ref=dst, send_sem=s, recv_sem=rcv, device_id=dev, device_id_type=MESH)

    mate_blocks = ((1 - chip_y) * 2 + (1 - core), chip_y * 2 + (1 - core))
    my_blocks = ((1 - chip_y) * 2 + core, chip_y * 2 + core)

    def a_stat(k):
        return remote(st_ref.at[mate_blocks[k]], got_st.at[k], as_s.at[k], as_r.at[k], mate)

    def a_copy(k, i):
        return remote(acc_ref.at[pl.ds(mate_blocks[k] * quarter + i * rc, rc)], got_acc.at[k, pl.ds(i * rc, rc)],
                      a_s.at[k, i], a_r.at[k, i], mate)

    for k in range(2):
        a_stat(k).start()
        for i in range(n_row):
            a_copy(k, i).start()

    lane = lax.broadcasted_iota(jnp.int32, (heads, 128), 1)

    def join(one, two):
        m_one, m_two = one, two
        top = jnp.maximum(m_one, m_two)
        f_one, f_two = jnp.exp(m_one - top), jnp.exp(m_two - top)
        l_one = pltpu.roll(one, 128 - quarter, 1)
        l_two = pltpu.roll(two, 128 - quarter, 1)
        total = l_one * f_one + l_two * f_two
        packed = jnp.where(lane < quarter, top, pltpu.roll(total, quarter, 1))
        return packed, f_one, f_two, total

    def b_stat():
        return remote(fwd_st, far_st, bs_s, bs_r, across)

    def b_copy(i):
        return remote(fwd_acc.at[pl.ds(i * rc, rc)], far_acc.at[pl.ds(i * rc, rc)], b_s.at[i], b_r.at[i], across)

    a_stat(0).wait()
    packed, f_one, f_two, _ = join(st_ref[my_blocks[0]], got_st[0])
    fwd_st[...] = packed
    b_stat().start()
    for i in range(n_row):
        a_copy(0, i).wait()
        mine_i = acc_ref[pl.ds(my_blocks[0] * quarter + i * rc, rc)]
        for b in range(rc):
            at = i * rc + b
            fwd_acc[at] = mine_i[b] * f_one[:, at:at + 1] + got_acc[0, at] * f_two[:, at:at + 1]
        b_copy(i).start()

    a_stat(1).wait()
    packed, f_one, f_two, _ = join(st_ref[my_blocks[1]], got_st[1])
    for i in range(n_row):
        a_copy(1, i).wait()
        mine_i = acc_ref[pl.ds(my_blocks[1] * quarter + i * rc, rc)]
        for b in range(rc):
            at = i * rc + b
            own_acc[at] = mine_i[b] * f_one[:, at:at + 1] + got_acc[1, at] * f_two[:, at:at + 1]

    b_stat().wait()
    _, g_one, g_two, total = join(packed, far_st[...])
    inv = 1.0 / jnp.where(lane < quarter, total, 1.0)
    g_one = g_one * inv
    g_two = g_two * inv

    load_x.wait()
    col_tile = lambda j: pl.ds(pl.multiple_of(j * cc, cc), cc)

    def finish(value, block, k):
        rows = pl.ds(pl.multiple_of(block * quarter + (k // n_col) * rc, rc), rc)
        cols = col_tile(lax.rem(k, n_col))
        y_ref[rows, cols] = (x_buf[rows, cols].astype(F32) + value + b_ref[:, cols].astype(F32)).astype(BF16)

    def x_copy(k):
        return remote(mine.at[k], near.at[k], x_s.at[k], x_r.at[k], inward)

    def p_copy(k):
        return remote(half.at[k], far_half.at[k], p_s.at[k], p_r.at[k], peer)

    def t_copy(k):
        return remote(tot.at[k], tot.at[k], t_s.at[k], t_r.at[k], outward)

    def y_copy(k):
        return remote(tot.at[k], from_y.at[k], y_s.at[k], y_r.at[k], across)

    def c_copy(k):
        return remote(tot.at[k], from_c.at[k], c_s.at[k], c_r.at[k], mate)

    def f_copy(k):
        return remote(from_y.at[k], from_yc.at[k], f_s.at[k], f_r.at[k], mate)

    def x_arrives(k):
        return remote(mine.at[k], near.at[k], x_s.at[k], x_r.at[k], outward)

    def t_arrives(k):
        return remote(tot.at[k], tot.at[k], t_s.at[k], t_r.at[k], inward)

    def spread(k):
        y_copy(k).start()
        c_copy(k).start()
        finish(tot[k], r, k)

    def at_lag(k, lag, do):
        if isinstance(k, int):
            if 0 <= k - lag < n:
                do(k - lag)
        else:
            pl.when((k >= lag) & (k - lag < n))(lambda: do(k - lag))

    def relay(k):
        y_copy(k).wait_recv()
        f_copy(k).start()
        finish(from_y[k], (1 - chip_y) * 2 + core, k)

    def collect(k):
        c_copy(k).wait_recv()
        finish(from_c[k], chip_y * 2 + 1 - core, k)
        f_copy(k).wait_recv()
        finish(from_yc[k], (1 - chip_y) * 2 + 1 - core, k)

    def total_inner(k):
        p_copy(k).wait_recv()
        tot[k] = half[k] + far_half[k]
        t_copy(k).start()
        spread(k)

    def total_outer(k):
        t_arrives(k).wait_recv()
        spread(k)

    def after(k):
        @pl.when(outer)
        def _():
            at_lag(k, LAGS_OUTER[0], total_outer)
            at_lag(k, LAGS_OUTER[1], relay)
            at_lag(k, LAGS_OUTER[2], collect)

        @pl.when(jnp.logical_not(outer))
        def _():
            at_lag(k, LAGS_INNER[0], total_inner)
            at_lag(k, LAGS_INNER[1], relay)
            at_lag(k, LAGS_INNER[2], collect)

    for i in range(n_row):
        b_copy(i).wait()
        for b in range(rc):
            at = i * rc + b
            own_acc[at] = own_acc[at] * g_one[:, at:at + 1] + far_acc[at] * g_two[:, at:at + 1]
        for h in range(heads):
            att[pl.ds(i * rc, rc), pl.ds(h * dim, dim)] = own_acc[pl.ds(i * rc, rc), h, :].astype(BF16)
        if i == 0:
            for cp in w_loads:
                cp.wait()

        @pl.loop(0, n_col)
        def _(j):
            k = i * n_col + j
            mine[k] = jnp.dot(att[i * rc:(i + 1) * rc], w_buf[:, col_tile(j)], preferred_element_type=F32)

            @pl.when(outer)
            def _():
                x_copy(k).start()

            @pl.when(jnp.logical_not(outer))
            def _():
                x_arrives(k).wait_recv()
                half[k] = mine[k] + near[k]
                p_copy(k).start()

            after(k)

    @pl.loop(n, n + max(LAGS_OUTER[2], LAGS_INNER[2]))
    def _(k):
        after(k)

    @pl.loop(0, n)
    def _(k):
        y_copy(k).wait_send()
        c_copy(k).wait_send()
        f_copy(k).wait_send()

        @pl.when(outer)
        def _():
            x_copy(k).wait_send()

        @pl.when(jnp.logical_not(outer))
        def _():
            p_copy(k).wait_send()
            t_copy(k).wait_send()


LAGS_INNER = (3, 6, 8)
LAGS_OUTER = (6, 9, 11)


def combine(acc, stat, tok_hidden, w_out, b_out, rc, cc):
    rows, heads, dim = acc.shape
    width = w_out.shape[1]
    quarter = rows // 4
    n_row, n_col = quarter // rc, width // cc
    n = n_row * n_col
    dma = pltpu.SemaphoreType.DMA
    part = pltpu.VMEM((quarter, heads, dim), F32)
    piece = pltpu.VMEM((n, rc, cc), F32)
    one_stat = pltpu.VMEM((heads, 128), F32)
    vmem = pl.BlockSpec(memory_space=pltpu.VMEM)
    hbm = pl.BlockSpec(memory_space=pl.ANY)
    return pl.pallas_call(
        functools.partial(combine_kernel, quarter, rc, cc),
        in_specs=[vmem, vmem, hbm, hbm, vmem],
        out_specs=vmem,
        out_shape=jax.ShapeDtypeStruct((rows, width), BF16),
        scratch_shapes=[
            pltpu.VMEM((2, quarter, heads, dim), F32), pltpu.VMEM((2, heads, 128), F32),
            part, one_stat, part, part, one_stat,
            pltpu.VMEM((quarter, heads * dim), BF16),
            pltpu.VMEM(w_out.shape, BF16), pltpu.VMEM((rows, width), BF16),
            *[piece] * 8,
            dma((1 + n_col,)),
            dma((2, n_row)), dma((2, n_row)), dma((2,)), dma((2,)),
            dma((n_row,)), dma((n_row,)), dma, dma,
            *[dma((n,))] * 12,
        ],
        compiler_params=pltpu.CompilerParams(collective_id=0, has_side_effects=True, vmem_limit_bytes=40 * 2**20),
    )(acc, stat, tok_hidden, w_out, b_out)


def solution(mesh):
    cache_spec = P('dp', 'tp', 'sp', None)
    row_spec = P('dp', None)

    def local_block(tok_hidden, cache_len, k_cache, v_cache, ln_gain, ln_bias, w_qkv, b_qkv, w_out, b_out):
        heads, dim, width = w_out.shape
        qkv = norm_project(tok_hidden, ln_gain, ln_bias, w_qkv, b_qkv)
        k_out, v_out, acc, stat = attend(qkv, cache_len, k_cache, v_cache, 16, tok_hidden.shape[0] // 4)
        y = combine(acc, stat, tok_hidden, w_out.reshape(heads * dim, width), b_out.reshape(1, width), 16, 1024)
        return y, k_out, v_out

    return jax.shard_map(
        local_block,
        mesh=mesh,
        in_specs=(row_spec, P('dp'), cache_spec, cache_spec, P(None), P(None), P(None, None, 'tp', None), P(None, 'tp', None), P('tp', None, None), P(None)),
        out_specs=(row_spec, cache_spec, cache_spec),
        check_vma=False,
    )
```

```python
import functools

import jax
import jax.numpy as jnp
from jax import lax
from jax.experimental import pallas as pl
from jax.experimental.pallas import tpu as pltpu
from jax.sharding import PartitionSpec as P

MESH = pl.DeviceIdType.MESH
NEG = float(jnp.finfo(jnp.float32).min)
F32 = jnp.float32
BF16 = jnp.bfloat16


def norm_project(tok_hidden, ln_gain, ln_bias, w_qkv, b_qkv):
    x_f32 = tok_hidden.astype(F32)
    mean_x = jnp.mean(x_f32, axis=-1, keepdims=True)
    centered = x_f32 - mean_x
    var_x = jnp.mean(centered * centered, axis=-1, keepdims=True)
    hidden = (centered * lax.rsqrt(var_x + 1e-5) * ln_gain + ln_bias).astype(BF16)
    qkv_all = jnp.einsum('bm,mthd->thbd', hidden, w_qkv, preferred_element_type=F32)
    return (qkv_all + b_qkv.astype(F32)[:, :, None, :]).astype(BF16)


def attend_kernel(slots, per_stat, len_ref, qkv_ref, k_ref, v_ref, ko_ref, vo_ref, acc_ref, st_ref, qkv_f32, scores, probs):
    rows, heads, _, dim = k_ref.shape
    step = pl.program_id(0)
    first = lax.axis_index('sp') * slots
    qkv_f32[...] = qkv_ref[...].astype(F32)
    slot = lax.broadcasted_iota(jnp.int32, (slots, dim), 0)
    flat = heads * slots
    row_id = lax.broadcasted_iota(jnp.int32, (heads, flat), 0)
    col_id = lax.broadcasted_iota(jnp.int32, (heads, flat), 1)
    in_head = (col_id // slots) == row_id
    col_slot = jnp.where(in_head, col_id % slots, slots)
    lane = lax.broadcasted_iota(jnp.int32, (heads, 128), 1)
    group = lax.rem(step, per_stat // rows)

    @pl.when(group == 0)
    def _():
        st_ref[...] = jnp.zeros_like(st_ref)

    local = [len_ref[step * rows + b] - first for b in range(rows)]
    for b in range(rows):
        hit = (slot == local[b])[None]
        k_new = jnp.broadcast_to(qkv_f32[1, :, b:b + 1, :], (heads, slots, dim)).astype(BF16)
        v_new = jnp.broadcast_to(qkv_f32[2, :, b:b + 1, :], (heads, slots, dim)).astype(BF16)
        k_all = jnp.where(hit, k_new, k_ref[b])
        ko_ref[b] = k_all
        vo_ref[b] = jnp.where(hit, v_new, v_ref[b])
        q = qkv_f32[0, :, b, :].astype(BF16)
        s = lax.dot_general(q, k_all.reshape(flat, dim), (((1,), (1,)), ((), ())), preferred_element_type=F32)
        scores[b] = jnp.where(col_slot <= jnp.minimum(local[b], slots - 1), s * dim ** -0.5, NEG)
    s = scores[...]
    top = jnp.max(s, axis=2, keepdims=True)
    w = jnp.where(s > NEG, jnp.exp(s - top), 0.0)
    total = jnp.sum(w, axis=2, keepdims=True)
    probs[...] = w.astype(BF16)
    stat = st_ref[0]
    for b in range(rows):
        at = group * rows + b
        stat = jnp.where(lane == at, top[b], stat)
        stat = jnp.where(lane == per_stat + at, total[b], stat)
        acc_ref[b] = jnp.dot(probs[b], vo_ref[b].reshape(flat, dim), preferred_element_type=F32)
    st_ref[0] = stat


def attend(qkv, cache_len, k_cache, v_cache, block, per_stat):
    rows, heads, slots, dim = k_cache.shape
    cache_block = pl.BlockSpec((block, heads, slots, dim), lambda i: (i, 0, 0, 0))
    return pl.pallas_call(
        functools.partial(attend_kernel, slots, per_stat),
        grid=(rows // block,),
        in_specs=[
            pl.BlockSpec(memory_space=pltpu.SMEM),
            pl.BlockSpec((3, heads, block, dim), lambda i: (0, 0, i, 0)),
            cache_block,
            cache_block,
        ],
        out_specs=[
            cache_block,
            cache_block,
            pl.BlockSpec((block, heads, dim), lambda i: (i, 0, 0)),
            pl.BlockSpec((1, heads, 128), lambda i: (i * block // per_stat, 0, 0)),
        ],
        out_shape=[
            jax.ShapeDtypeStruct(k_cache.shape, BF16),
            jax.ShapeDtypeStruct(v_cache.shape, BF16),
            jax.ShapeDtypeStruct((rows, heads, dim), F32),
            jax.ShapeDtypeStruct((rows // per_stat, heads, 128), F32),
        ],
        scratch_shapes=[
            pltpu.VMEM((3, heads, block, dim), F32),
            pltpu.VMEM((block, heads, heads * slots), F32),
            pltpu.VMEM((block, heads, heads * slots), BF16),
        ],
        compiler_params=pltpu.CompilerParams(dimension_semantics=("arbitrary",), vmem_limit_bytes=57 * 2**20),
    )(cache_len, qkv, k_cache, v_cache)


def combine_kernel(quarter, rc, cc, acc_ref, st_ref, x_hbm, w_hbm, b_ref, y_ref,
                   got_acc, got_st, fwd_acc, fwd_st, own_acc, far_acc, far_st, att,
                   w_buf, x_buf, mine, near, half, far_half, tot, from_y, from_c, from_yc, load_sem,
                   a_s, a_r, as_s, as_r, b_s, b_r, bs_s, bs_r,
                   x_s, x_r, p_s, p_r, t_s, t_r, y_s, y_r, c_s, c_r, f_s, f_r):
    heads, dim = acc_ref.shape[1:]
    n_row, n_col = quarter // rc, w_hbm.shape[1] // cc
    n = n_row * n_col
    r = lax.axis_index('sp')
    z = lax.axis_index('tp')
    core, chip_y = lax.rem(r, 2), r // 2
    mate = {'sp': chip_y * 2 + (1 - core)}
    across = {'sp': (1 - chip_y) * 2 + core}
    outer = (z == 0) | (z == 3)
    inward = {'tp': jnp.where(z == 0, 1, 2)}
    outward = {'tp': jnp.where(z == 1, 0, 3)}
    peer = {'tp': 3 - z}

    load_x = pltpu.make_async_copy(x_hbm, x_buf, load_sem.at[0])
    load_x.start()
    w_loads = []
    for j in range(n_col):
        cp = pltpu.make_async_copy(w_hbm.at[:, pl.ds(j * cc, cc)], w_buf.at[:, pl.ds(j * cc, cc)], load_sem.at[1 + j])
        cp.start()
        w_loads.append(cp)

    barrier = pltpu.get_barrier_semaphore()
    pl.semaphore_signal(barrier, inc=1, device_id=mate, device_id_type=MESH)
    pl.semaphore_signal(barrier, inc=1, device_id=across, device_id_type=MESH)

    @pl.when(outer)
    def _():
        pl.semaphore_signal(barrier, inc=1, device_id=inward, device_id_type=MESH)
        pl.semaphore_wait(barrier, 3)

    @pl.when(jnp.logical_not(outer))
    def _():
        pl.semaphore_signal(barrier, inc=1, device_id=outward, device_id_type=MESH)
        pl.semaphore_signal(barrier, inc=1, device_id=peer, device_id_type=MESH)
        pl.semaphore_wait(barrier, 4)

    def remote(src, dst, s, rcv, dev):
        return pltpu.make_async_remote_copy(src_ref=src, dst_ref=dst, send_sem=s, recv_sem=rcv, device_id=dev, device_id_type=MESH)

    mate_blocks = ((1 - chip_y) * 2 + (1 - core), chip_y * 2 + (1 - core))
    my_blocks = ((1 - chip_y) * 2 + core, chip_y * 2 + core)

    def a_stat(k):
        return remote(st_ref.at[mate_blocks[k]], got_st.at[k], as_s.at[k], as_r.at[k], mate)

    def a_copy(k, i):
        return remote(acc_ref.at[pl.ds(mate_blocks[k] * quarter + i * rc, rc)], got_acc.at[k, pl.ds(i * rc, rc)],
                      a_s.at[k, i], a_r.at[k, i], mate)

    for k in range(2):
        a_stat(k).start()
        for i in range(n_row):
            a_copy(k, i).start()

    lane = lax.broadcasted_iota(jnp.int32, (heads, 128), 1)

    def join(one, two):
        m_one, m_two = one, two
        top = jnp.maximum(m_one, m_two)
        f_one, f_two = jnp.exp(m_one - top), jnp.exp(m_two - top)
        l_one = pltpu.roll(one, 128 - quarter, 1)
        l_two = pltpu.roll(two, 128 - quarter, 1)
        total = l_one * f_one + l_two * f_two
        packed = jnp.where(lane < quarter, top, pltpu.roll(total, quarter, 1))
        return packed, f_one, f_two, total

    def b_stat():
        return remote(fwd_st, far_st, bs_s, bs_r, across)

    def b_copy(i):
        return remote(fwd_acc.at[pl.ds(i * rc, rc)], far_acc.at[pl.ds(i * rc, rc)], b_s.at[i], b_r.at[i], across)

    a_stat(0).wait()
    packed, f_one, f_two, _ = join(st_ref[my_blocks[0]], got_st[0])
    fwd_st[...] = packed
    b_stat().start()
    for i in range(n_row):
        a_copy(0, i).wait()
        mine_i = acc_ref[pl.ds(my_blocks[0] * quarter + i * rc, rc)]
        for b in range(rc):
            at = i * rc + b
            fwd_acc[at] = mine_i[b] * f_one[:, at:at + 1] + got_acc[0, at] * f_two[:, at:at + 1]
        b_copy(i).start()

    a_stat(1).wait()
    packed, f_one, f_two, _ = join(st_ref[my_blocks[1]], got_st[1])
    for i in range(n_row):
        a_copy(1, i).wait()
        mine_i = acc_ref[pl.ds(my_blocks[1] * quarter + i * rc, rc)]
        for b in range(rc):
            at = i * rc + b
            own_acc[at] = mine_i[b] * f_one[:, at:at + 1] + got_acc[1, at] * f_two[:, at:at + 1]

    b_stat().wait()
    _, g_one, g_two, total = join(packed, far_st[...])
    inv = 1.0 / jnp.where(lane < quarter, total, 1.0)
    g_one = g_one * inv
    g_two = g_two * inv

    load_x.wait()
    col_tile = lambda j: pl.ds(pl.multiple_of(j * cc, cc), cc)

    def finish(value, block, k):
        rows = pl.ds(pl.multiple_of(block * quarter + (k // n_col) * rc, rc), rc)
        cols = col_tile(lax.rem(k, n_col))
        y_ref[rows, cols] = (x_buf[rows, cols].astype(F32) + value + b_ref[:, cols].astype(F32)).astype(BF16)

    def x_copy(k):
        return remote(mine.at[k], near.at[k], x_s.at[k], x_r.at[k], inward)

    def p_copy(k):
        return remote(half.at[k], far_half.at[k], p_s.at[k], p_r.at[k], peer)

    def t_copy(k):
        return remote(tot.at[k], tot.at[k], t_s.at[k], t_r.at[k], outward)

    def y_copy(k):
        return remote(tot.at[k], from_y.at[k], y_s.at[k], y_r.at[k], across)

    def c_copy(k):
        return remote(tot.at[k], from_c.at[k], c_s.at[k], c_r.at[k], mate)

    def f_copy(k):
        return remote(from_y.at[k], from_yc.at[k], f_s.at[k], f_r.at[k], mate)

    def x_arrives(k):
        return remote(mine.at[k], near.at[k], x_s.at[k], x_r.at[k], outward)

    def t_arrives(k):
        return remote(tot.at[k], tot.at[k], t_s.at[k], t_r.at[k], inward)

    def spread(k):
        y_copy(k).start()
        c_copy(k).start()
        finish(tot[k], r, k)

    def at_lag(k, lag, do):
        if isinstance(k, int):
            if 0 <= k - lag < n:
                do(k - lag)
        else:
            pl.when((k >= lag) & (k - lag < n))(lambda: do(k - lag))

    def relay(k):
        y_copy(k).wait_recv()
        f_copy(k).start()
        finish(from_y[k], (1 - chip_y) * 2 + core, k)

    def collect(k):
        c_copy(k).wait_recv()
        finish(from_c[k], chip_y * 2 + 1 - core, k)
        f_copy(k).wait_recv()
        finish(from_yc[k], (1 - chip_y) * 2 + 1 - core, k)

    def total_inner(k):
        p_copy(k).wait_recv()
        tot[k] = half[k] + far_half[k]
        t_copy(k).start()
        spread(k)

    def total_outer(k):
        t_arrives(k).wait_recv()
        spread(k)

    def after(k):
        @pl.when(outer)
        def _():
            at_lag(k, LAGS_OUTER[0], total_outer)
            at_lag(k, LAGS_OUTER[1], relay)
            at_lag(k, LAGS_OUTER[2], collect)

        @pl.when(jnp.logical_not(outer))
        def _():
            at_lag(k, LAGS_INNER[0], total_inner)
            at_lag(k, LAGS_INNER[1], relay)
            at_lag(k, LAGS_INNER[2], collect)

    for i in range(n_row):
        b_copy(i).wait()
        for b in range(rc):
            at = i * rc + b
            own_acc[at] = own_acc[at] * g_one[:, at:at + 1] + far_acc[at] * g_two[:, at:at + 1]
        for h in range(heads):
            att[pl.ds(i * rc, rc), pl.ds(h * dim, dim)] = own_acc[pl.ds(i * rc, rc), h, :].astype(BF16)
        if i == 0:
            for cp in w_loads:
                cp.wait()

        @pl.loop(0, n_col)
        def _(j):
            k = i * n_col + j
            mine[k] = jnp.dot(att[i * rc:(i + 1) * rc], w_buf[:, col_tile(j)], preferred_element_type=F32)

            @pl.when(outer)
            def _():
                x_copy(k).start()

            @pl.when(jnp.logical_not(outer))
            def _():
                x_arrives(k).wait_recv()
                half[k] = mine[k] + near[k]
                p_copy(k).start()

            after(k)

    @pl.loop(n, n + max(LAGS_OUTER[2], LAGS_INNER[2]))
    def _(k):
        after(k)

    @pl.loop(0, n)
    def _(k):
        y_copy(k).wait_send()
        c_copy(k).wait_send()
        f_copy(k).wait_send()

        @pl.when(outer)
        def _():
            x_copy(k).wait_send()

        @pl.when(jnp.logical_not(outer))
        def _():
            p_copy(k).wait_send()
            t_copy(k).wait_send()


LAGS_INNER = (4, 8, 10)
LAGS_OUTER = (8, 12, 14)


def combine(acc, stat, tok_hidden, w_out, b_out, rc, cc):
    rows, heads, dim = acc.shape
    width = w_out.shape[1]
    quarter = rows // 4
    n_row, n_col = quarter // rc, width // cc
    n = n_row * n_col
    dma = pltpu.SemaphoreType.DMA
    part = pltpu.VMEM((quarter, heads, dim), F32)
    piece = pltpu.VMEM((n, rc, cc), F32)
    one_stat = pltpu.VMEM((heads, 128), F32)
    vmem = pl.BlockSpec(memory_space=pltpu.VMEM)
    hbm = pl.BlockSpec(memory_space=pltpu.HBM)
    return pl.pallas_call(
        functools.partial(combine_kernel, quarter, rc, cc),
        in_specs=[vmem, vmem, hbm, hbm, vmem],
        out_specs=vmem,
        out_shape=jax.ShapeDtypeStruct((rows, width), BF16),
        scratch_shapes=[
            pltpu.VMEM((2, quarter, heads, dim), F32), pltpu.VMEM((2, heads, 128), F32),
            part, one_stat, part, part, one_stat,
            pltpu.VMEM((quarter, heads * dim), BF16),
            pltpu.VMEM(w_out.shape, BF16), pltpu.VMEM((rows, width), BF16),
            *[piece] * 8,
            dma((1 + n_col,)),
            dma((2, n_row)), dma((2, n_row)), dma((2,)), dma((2,)),
            dma((n_row,)), dma((n_row,)), dma, dma,
            *[dma((n,))] * 12,
        ],
        compiler_params=pltpu.CompilerParams(collective_id=0, has_side_effects=True, vmem_limit_bytes=57 * 2**20),
    )(acc, stat, tok_hidden, w_out, b_out)


def solution(mesh):
    cache_spec = P('dp', 'tp', 'sp', None)
    row_spec = P('dp', None)

    def local_block(tok_hidden, cache_len, k_cache, v_cache, ln_gain, ln_bias, w_qkv, b_qkv, w_out, b_out):
        heads, dim, width = w_out.shape
        qkv = norm_project(tok_hidden, ln_gain, ln_bias, w_qkv, b_qkv)
        k_out, v_out, acc, stat = attend(qkv, cache_len, k_cache, v_cache, 32, tok_hidden.shape[0] // 4)
        y = combine(acc, stat, tok_hidden, w_out.reshape(heads * dim, width), b_out.reshape(1, width), 16, 1024)
        return y, k_out, v_out

    return jax.shard_map(
        local_block,
        mesh=mesh,
        in_specs=(row_spec, P('dp'), cache_spec, cache_spec, P(None), P(None), P(None, None, 'tp', None), P(None, 'tp', None), P('tp', None, None), P(None)),
        out_specs=(row_spec, cache_spec, cache_spec),
        check_vma=False,
    )
```

```python
import functools

import jax
import jax.numpy as jnp
from jax import lax
from jax.experimental import pallas as pl
from jax.experimental.pallas import tpu as pltpu
from jax.sharding import PartitionSpec as P

MESH = pl.DeviceIdType.MESH
NEG = float(jnp.finfo(jnp.float32).min)
F32 = jnp.float32
BF16 = jnp.bfloat16


def front_kernel(slots, mc, blk, per_stat, len_ref, x_hbm, gain_ref, bias_ref, w_hbm, bqkv_ref, k_hbm, v_hbm,
                 ko_hbm, vo_hbm, acc_ref, st_ref, x_buf, hid, w_buf, qkv, k_buf, v_buf, scores, probs,
                 x_sem, w_sem, k_sem, v_sem, ko_sem, vo_sem):
    rows, width = x_buf.shape
    heads, dim = acc_ref.shape[1:]
    ring = w_buf.shape[0]
    n_m = width // mc
    total = 3 * n_m
    n_blk = rows // blk
    first = lax.axis_index('sp') * slots

    def w_load(t, m, slot):
        return pltpu.make_async_copy(w_hbm.at[pl.ds(m * mc, mc), t], w_buf.at[slot], w_sem.at[slot])

    def cache_copies(i):
        part = pl.ds(i * blk, blk)
        return (pltpu.make_async_copy(k_hbm.at[part], k_buf.at[part], k_sem.at[i]),
                pltpu.make_async_copy(v_hbm.at[part], v_buf.at[part], v_sem.at[i]))

    def out_copies(i):
        part = pl.ds(i * blk, blk)
        return (pltpu.make_async_copy(k_buf.at[part], ko_hbm.at[part], ko_sem.at[i]),
                pltpu.make_async_copy(v_buf.at[part], vo_hbm.at[part], vo_sem.at[i]))

    load_x = pltpu.make_async_copy(x_hbm, x_buf, x_sem)
    load_x.start()
    for c in range(ring):
        w_load(c // n_m, c % n_m, c).start()
    load_x.wait()

    @pl.loop(0, rows // LN_ROWS)
    def _(i):
        part = pl.ds(pl.multiple_of(i * LN_ROWS, LN_ROWS), LN_ROWS)
        x = x_buf[part].astype(F32)
        mean = jnp.mean(x, axis=-1, keepdims=True)
        centered = x - mean
        var = jnp.mean(centered * centered, axis=-1, keepdims=True)
        hid[part] = (centered * lax.rsqrt(var + 1e-5) * gain_ref[...] + bias_ref[...]).astype(BF16)

    @pl.loop(0, 3)
    def _(t):
        bias = bqkv_ref[t].astype(F32)
        for m in range(n_m):
            c = t * n_m + m
            slot = lax.rem(c, ring)
            w_load(t, m, slot).wait()
            w = jnp.swapaxes(w_buf[slot], 0, 1)
            for h in range(0, heads, 2):
                r = jnp.dot(hid[:, m * mc:(m + 1) * mc], jnp.concatenate([w[h], w[h + 1]], axis=1), preferred_element_type=F32)
                for u in range(2):
                    part = r[:, u * dim:(u + 1) * dim]
                    if m:
                        part = qkv[t, h + u] + part
                    if m == n_m - 1:
                        part = (part + bias[h + u:h + u + 1]).astype(BF16).astype(F32)
                    qkv[t, h + u] = part
            ahead = m + ring

            @pl.when(c + ring < total)
            def _():
                w_load(t + ahead // n_m, ahead % n_m, slot).start()

            for j in range(ring):
                @pl.when(c + ring == total + j)
                def _():
                    for i in range(j * n_blk // ring, (j + 1) * n_blk // ring):
                        for cp in cache_copies(i):
                            cp.start()

    flat = heads * slots
    slot_id = lax.broadcasted_iota(jnp.int32, (slots, dim), 0)
    row_id = lax.broadcasted_iota(jnp.int32, (heads, flat), 0)
    col_id = lax.broadcasted_iota(jnp.int32, (heads, flat), 1)
    col_slot = jnp.where((col_id // slots) == row_id, col_id % slots, slots)
    lane = lax.broadcasted_iota(jnp.int32, (heads, 128), 1)

    @pl.loop(0, n_blk)
    def _(i):
        for cp in cache_copies(i):
            cp.wait()
        start = i * blk
        local = [len_ref[start + b] - first for b in range(blk)]
        for b in range(blk):
            at = start + b
            hit = (slot_id == local[b])[None]
            k_new = jnp.broadcast_to(qkv[1, :, pl.ds(at, 1), :], (heads, slots, dim)).astype(BF16)
            v_new = jnp.broadcast_to(qkv[2, :, pl.ds(at, 1), :], (heads, slots, dim)).astype(BF16)
            k_all = jnp.where(hit, k_new, k_buf[at])
            k_buf[at] = k_all
            v_buf[at] = jnp.where(hit, v_new, v_buf[at])
            q = qkv[0, :, pl.ds(at, 1), :].reshape(heads, dim).astype(BF16)
            s = lax.dot_general(q, k_all.reshape(flat, dim), (((1,), (1,)), ((), ())), preferred_element_type=F32)
            scores[b] = jnp.where(col_slot <= jnp.minimum(local[b], slots - 1), s * dim ** -0.5, NEG)
        s = scores[...]
        top = jnp.max(s, axis=2, keepdims=True)
        w = jnp.where(s > NEG, jnp.exp(s - top), 0.0)
        weight = jnp.sum(w, axis=2, keepdims=True)
        probs[...] = w.astype(BF16)
        group = lax.rem(start, per_stat)
        which = start // per_stat
        stat = st_ref[which]
        for b in range(blk):
            at = group + b
            stat = jnp.where(lane == at, top[b], stat)
            stat = jnp.where(lane == per_stat + at, weight[b], stat)
            acc_ref[start + b] = jnp.dot(probs[b], v_buf[start + b].reshape(flat, dim), preferred_element_type=F32)
        st_ref[which] = stat
        for cp in out_copies(i):
            cp.start()

    @pl.loop(0, n_blk)
    def _(i):
        for cp in out_copies(i):
            cp.wait()


LN_ROWS = 16


def front(tok_hidden, cache_len, k_cache, v_cache, ln_gain, ln_bias, w_qkv, b_qkv, mc, ring, blk, per_stat):
    rows, heads, slots, dim = k_cache.shape
    width = tok_hidden.shape[1]
    vmem = pl.BlockSpec(memory_space=pltpu.VMEM)
    hbm = pl.BlockSpec(memory_space=pltpu.HBM)
    dma = pltpu.SemaphoreType.DMA
    n_blk = rows // blk
    return pl.pallas_call(
        functools.partial(front_kernel, slots, mc, blk, per_stat),
        in_specs=[pl.BlockSpec(memory_space=pltpu.SMEM), hbm, vmem, vmem, hbm, vmem, hbm, hbm],
        out_specs=[hbm, hbm, vmem, vmem],
        out_shape=[
            jax.ShapeDtypeStruct(k_cache.shape, BF16),
            jax.ShapeDtypeStruct(v_cache.shape, BF16),
            pltpu.VMEM((rows, heads, dim), F32),
            pltpu.VMEM((rows // per_stat, heads, 128), F32),
        ],
        scratch_shapes=[
            pltpu.VMEM((rows, width), BF16), pltpu.VMEM((rows, width), BF16),
            pltpu.VMEM((ring, mc, heads, dim), BF16),
            pltpu.VMEM((3, heads, rows, dim), F32),
            pltpu.VMEM(k_cache.shape, BF16), pltpu.VMEM(v_cache.shape, BF16),
            pltpu.VMEM((blk, heads, heads * slots), F32), pltpu.VMEM((blk, heads, heads * slots), BF16),
            dma, dma((ring,)), dma((n_blk,)), dma((n_blk,)), dma((n_blk,)), dma((n_blk,)),
        ],
        compiler_params=pltpu.CompilerParams(vmem_limit_bytes=58 * 2**20),
    )(cache_len, tok_hidden, ln_gain.reshape(1, width), ln_bias.reshape(1, width), w_qkv, b_qkv, k_cache, v_cache)


def combine_kernel(quarter, rc, cc, acc_ref, st_ref, x_hbm, w_hbm, b_ref, y_ref,
                   got_acc, got_st, fwd_acc, fwd_st, own_acc, far_acc, far_st, att,
                   w_buf, x_buf, mine, near, half, far_half, tot, from_y, from_c, from_yc, load_sem,
                   a_s, a_r, as_s, as_r, b_s, b_r, bs_s, bs_r,
                   x_s, x_r, p_s, p_r, t_s, t_r, y_s, y_r, c_s, c_r, f_s, f_r):
    heads, dim = acc_ref.shape[1:]
    n_row, n_col = quarter // rc, w_hbm.shape[1] // cc
    n = n_row * n_col
    r = lax.axis_index('sp')
    z = lax.axis_index('tp')
    core, chip_y = lax.rem(r, 2), r // 2
    mate = {'sp': chip_y * 2 + (1 - core)}
    across = {'sp': (1 - chip_y) * 2 + core}
    outer = (z == 0) | (z == 3)
    inward = {'tp': jnp.where(z == 0, 1, 2)}
    outward = {'tp': jnp.where(z == 1, 0, 3)}
    peer = {'tp': 3 - z}

    load_x = pltpu.make_async_copy(x_hbm, x_buf, load_sem.at[0])
    load_x.start()
    w_loads = []
    for j in range(n_col):
        cp = pltpu.make_async_copy(w_hbm.at[:, pl.ds(j * cc, cc)], w_buf.at[:, pl.ds(j * cc, cc)], load_sem.at[1 + j])
        cp.start()
        w_loads.append(cp)

    barrier = pltpu.get_barrier_semaphore()
    pl.semaphore_signal(barrier, inc=1, device_id=mate, device_id_type=MESH)
    pl.semaphore_signal(barrier, inc=1, device_id=across, device_id_type=MESH)

    @pl.when(outer)
    def _():
        pl.semaphore_signal(barrier, inc=1, device_id=inward, device_id_type=MESH)
        pl.semaphore_wait(barrier, 3)

    @pl.when(jnp.logical_not(outer))
    def _():
        pl.semaphore_signal(barrier, inc=1, device_id=outward, device_id_type=MESH)
        pl.semaphore_signal(barrier, inc=1, device_id=peer, device_id_type=MESH)
        pl.semaphore_wait(barrier, 4)

    def remote(src, dst, s, rcv, dev):
        return pltpu.make_async_remote_copy(src_ref=src, dst_ref=dst, send_sem=s, recv_sem=rcv, device_id=dev, device_id_type=MESH)

    mate_blocks = ((1 - chip_y) * 2 + (1 - core), chip_y * 2 + (1 - core))
    my_blocks = ((1 - chip_y) * 2 + core, chip_y * 2 + core)

    def a_stat(k):
        return remote(st_ref.at[mate_blocks[k]], got_st.at[k], as_s.at[k], as_r.at[k], mate)

    def a_copy(k, i):
        return remote(acc_ref.at[pl.ds(mate_blocks[k] * quarter + i * rc, rc)], got_acc.at[k, pl.ds(i * rc, rc)],
                      a_s.at[k, i], a_r.at[k, i], mate)

    for k in range(2):
        a_stat(k).start()
        for i in range(n_row):
            a_copy(k, i).start()

    lane = lax.broadcasted_iota(jnp.int32, (heads, 128), 1)

    def join(one, two):
        m_one, m_two = one, two
        top = jnp.maximum(m_one, m_two)
        f_one, f_two = jnp.exp(m_one - top), jnp.exp(m_two - top)
        l_one = pltpu.roll(one, 128 - quarter, 1)
        l_two = pltpu.roll(two, 128 - quarter, 1)
        total = l_one * f_one + l_two * f_two
        packed = jnp.where(lane < quarter, top, pltpu.roll(total, quarter, 1))
        return packed, f_one, f_two, total

    def b_stat():
        return remote(fwd_st, far_st, bs_s, bs_r, across)

    def b_copy(i):
        return remote(fwd_acc.at[pl.ds(i * rc, rc)], far_acc.at[pl.ds(i * rc, rc)], b_s.at[i], b_r.at[i], across)

    a_stat(0).wait()
    packed, f_one, f_two, _ = join(st_ref[my_blocks[0]], got_st[0])
    fwd_st[...] = packed
    b_stat().start()
    for i in range(n_row):
        a_copy(0, i).wait()
        mine_i = acc_ref[pl.ds(my_blocks[0] * quarter + i * rc, rc)]
        for b in range(rc):
            at = i * rc + b
            fwd_acc[at] = mine_i[b] * f_one[:, at:at + 1] + got_acc[0, at] * f_two[:, at:at + 1]
        b_copy(i).start()

    a_stat(1).wait()
    packed, f_one, f_two, _ = join(st_ref[my_blocks[1]], got_st[1])
    for i in range(n_row):
        a_copy(1, i).wait()
        mine_i = acc_ref[pl.ds(my_blocks[1] * quarter + i * rc, rc)]
        for b in range(rc):
            at = i * rc + b
            own_acc[at] = mine_i[b] * f_one[:, at:at + 1] + got_acc[1, at] * f_two[:, at:at + 1]

    b_stat().wait()
    _, g_one, g_two, total = join(packed, far_st[...])
    inv = 1.0 / jnp.where(lane < quarter, total, 1.0)
    g_one = g_one * inv
    g_two = g_two * inv

    load_x.wait()
    col_tile = lambda j: pl.ds(pl.multiple_of(j * cc, cc), cc)

    def finish(value, block, k):
        rows = pl.ds(pl.multiple_of(block * quarter + (k // n_col) * rc, rc), rc)
        cols = col_tile(lax.rem(k, n_col))
        y_ref[rows, cols] = (x_buf[rows, cols].astype(F32) + value + b_ref[:, cols].astype(F32)).astype(BF16)

    def x_copy(k):
        return remote(mine.at[k], near.at[k], x_s.at[k], x_r.at[k], inward)

    def p_copy(k):
        return remote(half.at[k], far_half.at[k], p_s.at[k], p_r.at[k], peer)

    def t_copy(k):
        return remote(tot.at[k], tot.at[k], t_s.at[k], t_r.at[k], outward)

    def y_copy(k):
        return remote(tot.at[k], from_y.at[k], y_s.at[k], y_r.at[k], across)

    def c_copy(k):
        return remote(tot.at[k], from_c.at[k], c_s.at[k], c_r.at[k], mate)

    def f_copy(k):
        return remote(from_y.at[k], from_yc.at[k], f_s.at[k], f_r.at[k], mate)

    def x_arrives(k):
        return remote(mine.at[k], near.at[k], x_s.at[k], x_r.at[k], outward)

    def t_arrives(k):
        return remote(tot.at[k], tot.at[k], t_s.at[k], t_r.at[k], inward)

    def spread(k):
        y_copy(k).start()
        c_copy(k).start()
        finish(tot[k], r, k)

    def at_lag(k, lag, do):
        if isinstance(k, int):
            if 0 <= k - lag < n:
                do(k - lag)
        else:
            pl.when((k >= lag) & (k - lag < n))(lambda: do(k - lag))

    def relay(k):
        y_copy(k).wait_recv()
        f_copy(k).start()
        finish(from_y[k], (1 - chip_y) * 2 + core, k)

    def collect(k):
        c_copy(k).wait_recv()
        finish(from_c[k], chip_y * 2 + 1 - core, k)
        f_copy(k).wait_recv()
        finish(from_yc[k], (1 - chip_y) * 2 + 1 - core, k)

    def total_inner(k):
        p_copy(k).wait_recv()
        tot[k] = half[k] + far_half[k]
        t_copy(k).start()
        spread(k)

    def total_outer(k):
        t_arrives(k).wait_recv()
        spread(k)

    def after(k):
        @pl.when(outer)
        def _():
            at_lag(k, LAGS_OUTER[0], total_outer)
            at_lag(k, LAGS_OUTER[1], relay)
            at_lag(k, LAGS_OUTER[2], collect)

        @pl.when(jnp.logical_not(outer))
        def _():
            at_lag(k, LAGS_INNER[0], total_inner)
            at_lag(k, LAGS_INNER[1], relay)
            at_lag(k, LAGS_INNER[2], collect)

    for i in range(n_row):
        b_copy(i).wait()
        for b in range(rc):
            at = i * rc + b
            own_acc[at] = own_acc[at] * g_one[:, at:at + 1] + far_acc[at] * g_two[:, at:at + 1]
        for h in range(heads):
            att[pl.ds(i * rc, rc), pl.ds(h * dim, dim)] = own_acc[pl.ds(i * rc, rc), h, :].astype(BF16)
        if i == 0:
            for cp in w_loads:
                cp.wait()

        @pl.loop(0, n_col)
        def _(j):
            k = i * n_col + j
            mine[k] = jnp.dot(att[i * rc:(i + 1) * rc], w_buf[:, col_tile(j)], preferred_element_type=F32)

            @pl.when(outer)
            def _():
                x_copy(k).start()

            @pl.when(jnp.logical_not(outer))
            def _():
                x_arrives(k).wait_recv()
                half[k] = mine[k] + near[k]
                p_copy(k).start()

            after(k)

    @pl.loop(n, n + max(LAGS_OUTER[2], LAGS_INNER[2]))
    def _(k):
        after(k)

    @pl.loop(0, n)
    def _(k):
        y_copy(k).wait_send()
        c_copy(k).wait_send()
        f_copy(k).wait_send()

        @pl.when(outer)
        def _():
            x_copy(k).wait_send()

        @pl.when(jnp.logical_not(outer))
        def _():
            p_copy(k).wait_send()
            t_copy(k).wait_send()


LAGS_INNER = (4, 8, 10)
LAGS_OUTER = (8, 12, 14)


def combine(acc, stat, tok_hidden, w_out, b_out, rc, cc):
    rows, heads, dim = acc.shape
    width = w_out.shape[1]
    quarter = rows // 4
    n_row, n_col = quarter // rc, width // cc
    n = n_row * n_col
    dma = pltpu.SemaphoreType.DMA
    part = pltpu.VMEM((quarter, heads, dim), F32)
    piece = pltpu.VMEM((n, rc, cc), F32)
    one_stat = pltpu.VMEM((heads, 128), F32)
    vmem = pl.BlockSpec(memory_space=pltpu.VMEM)
    hbm = pl.BlockSpec(memory_space=pltpu.HBM)
    return pl.pallas_call(
        functools.partial(combine_kernel, quarter, rc, cc),
        in_specs=[vmem, vmem, hbm, hbm, vmem],
        out_specs=vmem,
        out_shape=pltpu.VMEM((rows, width), BF16),
        scratch_shapes=[
            pltpu.VMEM((2, quarter, heads, dim), F32), pltpu.VMEM((2, heads, 128), F32),
            part, one_stat, part, part, one_stat,
            pltpu.VMEM((quarter, heads * dim), BF16),
            pltpu.VMEM(w_out.shape, BF16), pltpu.VMEM((rows, width), BF16),
            *[piece] * 8,
            dma((1 + n_col,)),
            dma((2, n_row)), dma((2, n_row)), dma((2,)), dma((2,)),
            dma((n_row,)), dma((n_row,)), dma, dma,
            *[dma((n,))] * 12,
        ],
        compiler_params=pltpu.CompilerParams(collective_id=0, has_side_effects=True, vmem_limit_bytes=54 * 2**20),
    )(acc, stat, tok_hidden, w_out, b_out)


def solution(mesh):
    cache_spec = P('dp', 'tp', 'sp', None)
    row_spec = P('dp', None)

    def local_block(tok_hidden, cache_len, k_cache, v_cache, ln_gain, ln_bias, w_qkv, b_qkv, w_out, b_out):
        heads, dim, width = w_out.shape
        k_out, v_out, acc, stat = front(tok_hidden, cache_len, k_cache, v_cache, ln_gain, ln_bias, w_qkv, b_qkv,
                                        2048, 3, 32, tok_hidden.shape[0] // 4)
        y = combine(acc, stat, tok_hidden, w_out.reshape(heads * dim, width), b_out.reshape(1, width), 16, 1024)
        return y, k_out, v_out

    return jax.shard_map(
        local_block,
        mesh=mesh,
        in_specs=(row_spec, P('dp'), cache_spec, cache_spec, P(None), P(None), P(None, None, 'tp', None), P(None, 'tp', None), P('tp', None, None), P(None)),
        out_specs=(row_spec, cache_spec, cache_spec),
        check_vma=False,
    )
```

```python
import functools

import jax
import jax.numpy as jnp
from jax import lax
from jax.experimental import pallas as pl
from jax.experimental.pallas import tpu as pltpu
from jax.sharding import PartitionSpec as P

MESH = pl.DeviceIdType.MESH
NEG = float(jnp.finfo(jnp.float32).min)
F32 = jnp.float32
BF16 = jnp.bfloat16


def front_kernel(slots, mc, blk, len_hbm, x_hbm, gain_hbm, bias_hbm, w_hbm, bqkv_hbm, k_hbm, v_hbm,
                 ko_hbm, vo_hbm, k_buf, v_buf, qkv, len_ref, gain_ref, bias_ref, bqkv_ref, x_buf, hid, w_buf,
                 small_sem, x_sem, w_sem, k_sem, v_sem, ko_sem, vo_sem):
    rows, width = x_buf.shape
    heads, dim = qkv.shape[1], qkv.shape[3]
    ring = w_buf.shape[0]
    n_m = width // mc
    total = 3 * n_m
    n_blk = rows // blk
    first = lax.axis_index('sp') * slots

    def w_load(t, m, slot):
        return pltpu.make_async_copy(w_hbm.at[pl.ds(m * mc, mc), t], w_buf.at[slot], w_sem.at[slot])

    def cache_copies(i):
        part = pl.ds(i * blk, blk)
        return (pltpu.make_async_copy(k_hbm.at[part], k_buf.at[part], k_sem.at[i]),
                pltpu.make_async_copy(v_hbm.at[part], v_buf.at[part], v_sem.at[i]))

    def out_copies(i):
        part = pl.ds(i * blk, blk)
        return (pltpu.make_async_copy(k_buf.at[part], ko_hbm.at[part], ko_sem.at[i]),
                pltpu.make_async_copy(v_buf.at[part], vo_hbm.at[part], vo_sem.at[i]))

    load_x = pltpu.make_async_copy(x_hbm, x_buf, x_sem)
    load_x.start()
    small = [pltpu.make_async_copy(src, dst, small_sem.at[n]) for n, (src, dst) in enumerate(
        ((gain_hbm, gain_ref), (bias_hbm, bias_ref), (bqkv_hbm, bqkv_ref), (len_hbm, len_ref)))]
    for cp in small:
        cp.start()
    for c in range(ring):
        w_load(c // n_m, c % n_m, c).start()
    load_x.wait()
    for cp in small:
        cp.wait()

    @pl.loop(0, rows // LN_ROWS)
    def _(i):
        part = pl.ds(pl.multiple_of(i * LN_ROWS, LN_ROWS), LN_ROWS)
        x = x_buf[part].astype(F32)
        mean = jnp.mean(x, axis=-1, keepdims=True)
        centered = x - mean
        var = jnp.mean(centered * centered, axis=-1, keepdims=True)
        hid[part] = (centered * lax.rsqrt(var + 1e-5) * gain_ref[...] + bias_ref[...]).astype(BF16)
        per = n_blk // EARLY

        @pl.when(i < EARLY)
        def _():
            for u in range(per):
                for cp in cache_copies(i * per + u):
                    cp.start()

    @pl.loop(0, 3)
    def _(t):
        bias = bqkv_ref[t].astype(F32)
        for m in range(n_m):
            c = t * n_m + m
            slot = lax.rem(c, ring)
            w_load(t, m, slot).wait()
            w = jnp.swapaxes(w_buf[slot], 0, 1)
            for h in range(0, heads, 2):
                r = jnp.dot(hid[:, m * mc:(m + 1) * mc], jnp.concatenate([w[h], w[h + 1]], axis=1), preferred_element_type=F32)
                for u in range(2):
                    part = r[:, u * dim:(u + 1) * dim]
                    if m:
                        part = qkv[t, h + u] + part
                    if m == n_m - 1:
                        part = (part + bias[h + u:h + u + 1]).astype(BF16).astype(F32)
                    qkv[t, h + u] = part
            ahead = m + ring

            @pl.when(c + ring < total)
            def _():
                w_load(t + ahead // n_m, ahead % n_m, slot).start()

    slot_id = lax.broadcasted_iota(jnp.int32, (slots, dim), 0)

    @pl.loop(0, n_blk)
    def _(i):
        for cp in cache_copies(i):
            cp.wait()
        for b in range(blk):
            at = i * blk + b
            hit = (slot_id == len_ref[at] - first)[None]
            for t, buf in ((1, k_buf), (2, v_buf)):
                new = jnp.broadcast_to(qkv[t, :, pl.ds(at, 1), :], (heads, slots, dim)).astype(BF16)
                buf[at] = jnp.where(hit, new, buf[at])
        for cp in out_copies(i):
            cp.start()

    @pl.loop(0, n_blk)
    def _(i):
        for cp in out_copies(i):
            cp.wait()


LN_ROWS = 64
EARLY = 4


def in_hbm(*arrays):
    return [pltpu.with_memory_space_constraint(a, pltpu.HBM) for a in arrays]


def front(tok_hidden, cache_len, k_cache, v_cache, ln_gain, ln_bias, w_qkv, b_qkv, mc, ring, blk):
    rows, heads, slots, dim = k_cache.shape
    width = tok_hidden.shape[1]
    vmem = pl.BlockSpec(memory_space=pltpu.VMEM)
    hbm = pl.BlockSpec(memory_space=pltpu.HBM)
    dma = pltpu.SemaphoreType.DMA
    n_blk = rows // blk
    return pl.pallas_call(
        functools.partial(front_kernel, slots, mc, blk),
        in_specs=[hbm] * 8,
        out_specs=[hbm, hbm, vmem, vmem, vmem],
        out_shape=[
            jax.ShapeDtypeStruct(k_cache.shape, BF16),
            jax.ShapeDtypeStruct(v_cache.shape, BF16),
            pltpu.VMEM(k_cache.shape, BF16),
            pltpu.VMEM(v_cache.shape, BF16),
            pltpu.VMEM((3, heads, rows, dim), F32),
        ],
        scratch_shapes=[
            pltpu.SMEM((rows,), jnp.int32), pltpu.VMEM((1, width), F32), pltpu.VMEM((1, width), F32), pltpu.VMEM(b_qkv.shape, BF16),
            pltpu.VMEM((rows, width), BF16), pltpu.VMEM((rows, width), BF16),
            pltpu.VMEM((ring, mc, heads, dim), BF16),
            dma((4,)), dma, dma((ring,)), dma((n_blk,)), dma((n_blk,)), dma((n_blk,)), dma((n_blk,)),
        ],
        compiler_params=pltpu.CompilerParams(vmem_limit_bytes=34 * 2**20),
    )(*in_hbm(cache_len, tok_hidden, ln_gain.reshape(1, width), ln_bias.reshape(1, width), w_qkv, b_qkv, k_cache, v_cache))


def combine_kernel(quarter, rc, cc, len_hbm, qkv_ref, k_ref, v_ref, x_hbm, w_hbm, b_hbm, y_ref, len_ref, b_tiles, b_ref,
                   acc_ref, st_ref, scores, probs, got_acc, got_st, fwd_acc, fwd_st, own_acc, own_st, far_acc, far_st, att,
                   w_buf, x_buf, mine, near, half, far_half, tot, from_y, from_c, from_yc, load_sem, len_sem, b_sem,
                   a_s, a_r, as_s, as_r, b_s, b_r, bs_s, bs_r,
                   x_s, x_r, p_s, p_r, t_s, t_r, y_s, y_r, c_s, c_r, f_s, f_r):
    heads, slots, dim = k_ref.shape[1:]
    n_row, n_col = quarter // rc, w_hbm.shape[1] // cc
    n = n_row * n_col
    r = lax.axis_index('sp')
    z = lax.axis_index('tp')
    core, chip_y = lax.rem(r, 2), r // 2
    mate = {'sp': chip_y * 2 + (1 - core)}
    across = {'sp': (1 - chip_y) * 2 + core}
    outer = (z == 0) | (z == 3)
    inward = {'tp': jnp.where(z == 0, 1, 2)}
    outward = {'tp': jnp.where(z == 1, 0, 3)}
    peer = {'tp': 3 - z}

    load_len = pltpu.make_async_copy(len_hbm, len_ref, len_sem)
    load_len.start()
    load_b = pltpu.make_async_copy(b_hbm, b_tiles, b_sem)
    load_b.start()
    load_x = pltpu.make_async_copy(x_hbm, x_buf, load_sem.at[0])
    load_x.start()
    w_loads = []
    for j in range(n_col):
        cp = pltpu.make_async_copy(w_hbm.at[:, pl.ds(j * cc, cc)], w_buf.at[:, pl.ds(j * cc, cc)], load_sem.at[1 + j])
        cp.start()
        w_loads.append(cp)

    barrier = pltpu.get_barrier_semaphore()
    pl.semaphore_signal(barrier, inc=1, device_id=mate, device_id_type=MESH)
    pl.semaphore_signal(barrier, inc=1, device_id=across, device_id_type=MESH)

    @pl.when(outer)
    def _():
        pl.semaphore_signal(barrier, inc=1, device_id=inward, device_id_type=MESH)
        pl.semaphore_wait(barrier, 3)

    @pl.when(jnp.logical_not(outer))
    def _():
        pl.semaphore_signal(barrier, inc=1, device_id=outward, device_id_type=MESH)
        pl.semaphore_signal(barrier, inc=1, device_id=peer, device_id_type=MESH)
        pl.semaphore_wait(barrier, 4)

    def remote(src, dst, s, rcv, dev):
        return pltpu.make_async_remote_copy(src_ref=src, dst_ref=dst, send_sem=s, recv_sem=rcv, device_id=dev, device_id_type=MESH)

    mate_blocks = ((1 - chip_y) * 2 + (1 - core), chip_y * 2 + (1 - core))
    my_blocks = ((1 - chip_y) * 2 + core, chip_y * 2 + core)

    def a_stat(k, i):
        return remote(st_ref.at[i, mate_blocks[k]], got_st.at[k, i], as_s.at[k, i], as_r.at[k, i], mate)

    def a_copy(k, i):
        return remote(acc_ref.at[pl.ds(mate_blocks[k] * quarter + i * rc, rc)], got_acc.at[k, pl.ds(i * rc, rc)],
                      a_s.at[k, i], a_r.at[k, i], mate)

    load_len.wait()
    load_b.wait()
    bias = b_tiles[...].astype(F32)
    for j in range(bias.shape[0]):
        b_ref[:, j * 128:(j + 1) * 128] = bias[j:j + 1]
    lane = lax.broadcasted_iota(jnp.int32, (heads, 128), 1)

    def join(one, two):
        m_one, m_two = one, two
        top = jnp.maximum(m_one, m_two)
        f_one, f_two = jnp.exp(m_one - top), jnp.exp(m_two - top)
        l_one = pltpu.roll(one, 128 - quarter, 1)
        l_two = pltpu.roll(two, 128 - quarter, 1)
        total = l_one * f_one + l_two * f_two
        packed = jnp.where(lane < quarter, top, pltpu.roll(total, quarter, 1))
        return packed, f_one, f_two, total

    def b_stat(i):
        return remote(fwd_st.at[i], far_st.at[i], bs_s.at[i], bs_r.at[i], across)

    def b_copy(i):
        return remote(fwd_acc.at[pl.ds(i * rc, rc)], far_acc.at[pl.ds(i * rc, rc)], b_s.at[i], b_r.at[i], across)

    first = r * slots
    flat = heads * slots
    row_id = lax.broadcasted_iota(jnp.int32, (heads, flat), 0)
    col_id = lax.broadcasted_iota(jnp.int32, (heads, flat), 1)
    col_slot = jnp.where((col_id // slots) == row_id, col_id % slots, slots)
    places = [(j, b) for j in range(4) for b in range(rc)]

    def attend(i):
        for n_at, (j, b) in enumerate(places):
            at = j * quarter + i * rc + b
            q = qkv_ref[0, :, pl.ds(at, 1), :].reshape(heads, dim).astype(BF16)
            s = lax.dot_general(q, k_ref[at].reshape(flat, dim), (((1,), (1,)), ((), ())), preferred_element_type=F32)
            scores[n_at] = jnp.where(col_slot <= jnp.minimum(len_ref[at] - first, slots - 1), s * dim ** -0.5, NEG)
        s = scores[...]
        top = jnp.max(s, axis=2, keepdims=True)
        w = jnp.where(s > NEG, jnp.exp(s - top), 0.0)
        weight = jnp.sum(w, axis=2, keepdims=True)
        probs[...] = w.astype(BF16)
        for j in range(4):
            stat = jnp.zeros((heads, 128), F32)
            for b in range(rc):
                stat = jnp.where(lane == b, top[j * rc + b], stat)
                stat = jnp.where(lane == quarter + b, weight[j * rc + b], stat)
            st_ref[i, j] = stat
        for n_at, (j, b) in enumerate(places):
            at = j * quarter + i * rc + b
            acc_ref[at] = jnp.dot(probs[n_at], v_ref[at].reshape(flat, dim), preferred_element_type=F32)
        for k in range(2):
            a_stat(k, i).start()
            a_copy(k, i).start()

    def join_core(i):
        for k in range(2):
            a_stat(k, i).wait()
            a_copy(k, i).wait()
            packed, f_one, f_two, _ = join(st_ref[i, my_blocks[k]], got_st[k, i])
            for b in range(rc):
                at = i * rc + b
                value = acc_ref[my_blocks[k] * quarter + at] * f_one[:, b:b + 1] + got_acc[k, at] * f_two[:, b:b + 1]
                if k == 0:
                    fwd_acc[at] = value
                else:
                    own_acc[at] = value
            if k == 0:
                fwd_st[i] = packed
                b_stat(i).start()
                b_copy(i).start()
            else:
                own_st[i] = packed

    def join_chips(i):
        b_stat(i).wait()
        b_copy(i).wait()
        _, g_one, g_two, total = join(own_st[i], far_st[i])
        inv = 1.0 / jnp.where(lane < rc, total, 1.0)
        g_one = g_one * inv
        g_two = g_two * inv
        for b in range(rc):
            at = i * rc + b
            own_acc[at] = own_acc[at] * g_one[:, b:b + 1] + far_acc[at] * g_two[:, b:b + 1]
        for h in range(heads):
            att[i, :, pl.ds(h * dim, dim)] = own_acc[pl.ds(i * rc, rc), h, :].astype(BF16)

    col_tile = lambda j: pl.ds(pl.multiple_of(j * cc, cc), cc)

    def finish(value, block, k):
        rows = pl.ds(pl.multiple_of(block * quarter + (k // n_col) * rc, rc), rc)
        cols = col_tile(lax.rem(k, n_col))
        y_ref[rows, cols] = (x_buf[rows, cols].astype(F32) + value + b_ref[:, cols]).astype(BF16)

    def x_copy(k):
        return remote(mine.at[k], near.at[k], x_s.at[k], x_r.at[k], inward)

    def p_copy(k):
        return remote(half.at[k], far_half.at[k], p_s.at[k], p_r.at[k], peer)

    def t_copy(k):
        return remote(tot.at[k], tot.at[k], t_s.at[k], t_r.at[k], outward)

    def y_copy(k):
        return remote(tot.at[k], from_y.at[k], y_s.at[k], y_r.at[k], across)

    def c_copy(k):
        return remote(tot.at[k], from_c.at[k], c_s.at[k], c_r.at[k], mate)

    def f_copy(k):
        return remote(from_y.at[k], from_yc.at[k], f_s.at[k], f_r.at[k], mate)

    def x_arrives(k):
        return remote(mine.at[k], near.at[k], x_s.at[k], x_r.at[k], outward)

    def t_arrives(k):
        return remote(tot.at[k], tot.at[k], t_s.at[k], t_r.at[k], inward)

    def spread(k):
        y_copy(k).start()
        c_copy(k).start()
        finish(tot[k], r, k)

    def at_lag(k, lag, do):
        if isinstance(k, int):
            if 0 <= k - lag < n:
                do(k - lag)
        else:
            pl.when((k >= lag) & (k - lag < n))(lambda: do(k - lag))

    def relay(k):
        y_copy(k).wait_recv()
        f_copy(k).start()
        finish(from_y[k], (1 - chip_y) * 2 + core, k)

    def collect(k):
        c_copy(k).wait_recv()
        finish(from_c[k], chip_y * 2 + 1 - core, k)
        f_copy(k).wait_recv()
        finish(from_yc[k], (1 - chip_y) * 2 + 1 - core, k)

    def total_inner(k):
        p_copy(k).wait_recv()
        tot[k] = half[k] + far_half[k]
        t_copy(k).start()
        spread(k)

    def total_outer(k):
        t_arrives(k).wait_recv()
        spread(k)

    def half_inner(k):
        x_arrives(k).wait_recv()
        half[k] = mine[k] + near[k]
        p_copy(k).start()

    def after(k):
        @pl.when(outer)
        def _():
            at_lag(k, LAGS_OUTER[0], total_outer)
            at_lag(k, LAGS_OUTER[1], relay)
            at_lag(k, LAGS_OUTER[2], collect)

        @pl.when(jnp.logical_not(outer))
        def _():
            at_lag(k, LAG_HALF, half_inner)
            at_lag(k, LAGS_INNER[0], total_inner)
            at_lag(k, LAGS_INNER[1], relay)
            at_lag(k, LAGS_INNER[2], collect)

    @pl.loop(0, n_row + LAG_CHIPS)
    def _(i):
        @pl.when(i < n_row)
        def _():
            attend(i)

        @pl.when((i >= LAG_CORE) & (i - LAG_CORE < n_row))
        def _():
            join_core(i - LAG_CORE)

        @pl.when(i == LAG_CHIPS)
        def _():
            load_x.wait()
            for cp in w_loads:
                cp.wait()

        @pl.when(i >= LAG_CHIPS)
        def _():
            row = i - LAG_CHIPS
            join_chips(row)

            @pl.loop(0, n_col)
            def _(j):
                k = row * n_col + j
                mine[k] = jnp.dot(att[row], w_buf[:, col_tile(j)], preferred_element_type=F32)

                @pl.when(outer)
                def _():
                    x_copy(k).start()

                after(k)

    @pl.loop(n, n + max(LAGS_OUTER[2], LAGS_INNER[2]))
    def _(k):
        after(k)

    @pl.loop(0, n)
    def _(k):
        y_copy(k).wait_send()
        c_copy(k).wait_send()
        f_copy(k).wait_send()

        @pl.when(outer)
        def _():
            x_copy(k).wait_send()

        @pl.when(jnp.logical_not(outer))
        def _():
            p_copy(k).wait_send()
            t_copy(k).wait_send()


LAG_CORE = 1
LAG_CHIPS = 2
LAG_HALF = 2
LAGS_INNER = (5, 9, 11)
LAGS_OUTER = (16, 20, 22)


def combine(cache_len, qkv, k_new, v_new, tok_hidden, w_out, b_out, rc, cc):
    rows, heads, slots, dim = k_new.shape
    width = w_out.shape[1]
    quarter = rows // 4
    n_row, n_col = quarter // rc, width // cc
    n = n_row * n_col
    dma = pltpu.SemaphoreType.DMA
    part = pltpu.VMEM((quarter, heads, dim), F32)
    piece = pltpu.VMEM((n, rc, cc), F32)
    stat = pltpu.VMEM((n_row, heads, 128), F32)
    qkv, k_new, v_new = (pltpu.with_memory_space_constraint(a, pltpu.VMEM) for a in (qkv, k_new, v_new))
    vmem = pl.BlockSpec(memory_space=pltpu.VMEM)
    hbm = pl.BlockSpec(memory_space=pltpu.HBM)
    return pl.pallas_call(
        functools.partial(combine_kernel, quarter, rc, cc),
        in_specs=[hbm, vmem, vmem, vmem, hbm, hbm, hbm],
        out_specs=vmem,
        out_shape=pltpu.VMEM((rows, width), BF16),
        scratch_shapes=[
            pltpu.SMEM((rows,), jnp.int32), pltpu.VMEM(b_out.shape, BF16), pltpu.VMEM((1, width), F32),
            pltpu.VMEM((rows, heads, dim), F32), pltpu.VMEM((n_row, 4, heads, 128), F32),
            pltpu.VMEM((4 * rc, heads, heads * slots), F32), pltpu.VMEM((4 * rc, heads, heads * slots), BF16),
            pltpu.VMEM((2, quarter, heads, dim), F32), pltpu.VMEM((2, n_row, heads, 128), F32),
            part, stat, part, stat, part, stat,
            pltpu.VMEM((n_row, rc, heads * dim), BF16),
            pltpu.VMEM(w_out.shape, BF16), pltpu.VMEM((rows, width), BF16),
            *[piece] * 8,
            dma((1 + n_col,)), dma, dma,
            *[dma((2, n_row))] * 4,
            *[dma((n_row,))] * 4,
            *[dma((n,))] * 12,
        ],
        compiler_params=pltpu.CompilerParams(collective_id=0, has_side_effects=True, vmem_limit_bytes=30 * 2**20),
    )(*in_hbm(cache_len), qkv, k_new, v_new, *in_hbm(tok_hidden, w_out, b_out))


def solution(mesh):
    cache_spec = P('dp', 'tp', 'sp', None)
    row_spec = P('dp', None)

    def local_block(tok_hidden, cache_len, k_cache, v_cache, ln_gain, ln_bias, w_qkv, b_qkv, w_out, b_out):
        heads, dim, width = w_out.shape
        k_out, v_out, k_new, v_new, qkv = front(tok_hidden, cache_len, k_cache, v_cache, ln_gain, ln_bias, w_qkv, b_qkv, 2048, 3, 32)
        y = combine(cache_len, qkv, k_new, v_new, tok_hidden, w_out.reshape(heads * dim, width), b_out.reshape(width // 128, 128), 16, 1024)
        return y, k_out, v_out

    return jax.shard_map(
        local_block,
        mesh=mesh,
        in_specs=(row_spec, P('dp'), cache_spec, cache_spec, P(None), P(None), P(None, None, 'tp', None), P(None, 'tp', None), P('tp', None, None), P(None)),
        out_specs=(row_spec, cache_spec, cache_spec),
        check_vma=False,
    )
```

```python
import functools

import jax
import jax.numpy as jnp
from jax import lax
from jax.experimental import pallas as pl
from jax.experimental.pallas import tpu as pltpu
from jax.sharding import PartitionSpec as P

MESH = pl.DeviceIdType.MESH
NEG = float(jnp.finfo(jnp.float32).min)
F32 = jnp.float32
BF16 = jnp.bfloat16


def attend_rows(places, row_at, slots, rc, len_ref, first, qkv_ref, k_ref, v_ref, scores, probs, put_stat, put_acc):
    heads, dim = k_ref.shape[1], k_ref.shape[3]
    flat = heads * slots
    row_id = lax.broadcasted_iota(jnp.int32, (heads, flat), 0)
    col_id = lax.broadcasted_iota(jnp.int32, (heads, flat), 1)
    col_slot = jnp.where((col_id // slots) == row_id, col_id % slots, slots)
    lane = lax.broadcasted_iota(jnp.int32, (heads, 128), 1)
    for n_at, (j, b) in enumerate(places):
        at = row_at(j, b)
        q = qkv_ref[0, :, pl.ds(at, 1), :].reshape(heads, dim).astype(BF16)
        s = lax.dot_general(q, k_ref[at].reshape(flat, dim), (((1,), (1,)), ((), ())), preferred_element_type=F32)
        scores[n_at] = jnp.where(col_slot <= jnp.minimum(len_ref[at] - first, slots - 1), s * dim ** -0.5, NEG)
    s = scores[...]
    top = jnp.max(s, axis=2, keepdims=True)
    w = jnp.where(s > NEG, jnp.exp(s - top), 0.0)
    weight = jnp.sum(w, axis=2, keepdims=True)
    probs[...] = w.astype(BF16)
    for j in range(4):
        m_tile = l_tile = jnp.zeros((heads, 128), F32)
        for b in range(rc):
            m_tile = jnp.where(lane == b, top[j * rc + b], m_tile)
            l_tile = jnp.where(lane == b, weight[j * rc + b], l_tile)
        put_stat(j, m_tile, l_tile)
    for n_at, (j, b) in enumerate(places):
        put_acc(j, b, jnp.dot(probs[n_at], v_ref[row_at(j, b)].reshape(flat, dim), preferred_element_type=F32))


def places_of(rc):
    return [(j, b) for j in range(4) for b in range(rc)]


def front_kernel(slots, mc, blk, rc, len_hbm, x_hbm, gain_hbm, bias_hbm, w_hbm, bqkv_hbm, k_hbm, v_hbm,
                 ko_hbm, vo_hbm, k_buf, v_buf, qkv, acc0, st0, scores, probs, len_ref, gain_ref, bias_ref, bqkv_ref, x_buf, hid, w_buf,
                 small_sem, x_sem, w_sem, k_sem, v_sem, ko_sem, vo_sem):
    rows, width = x_buf.shape
    heads, dim = qkv.shape[1], qkv.shape[3]
    ring = w_buf.shape[0]
    n_m = width // mc
    total = 3 * n_m
    n_blk = rows // blk
    first = lax.axis_index('sp') * slots

    def w_load(t, m, slot):
        return pltpu.make_async_copy(w_hbm.at[pl.ds(m * mc, mc), t], w_buf.at[slot], w_sem.at[slot])

    def cache_copies(i):
        part = pl.ds(i * blk, blk)
        return (pltpu.make_async_copy(k_hbm.at[part], k_buf.at[part], k_sem.at[i]),
                pltpu.make_async_copy(v_hbm.at[part], v_buf.at[part], v_sem.at[i]))

    def out_copies(i):
        part = pl.ds(i * blk, blk)
        return (pltpu.make_async_copy(k_buf.at[part], ko_hbm.at[part], ko_sem.at[i]),
                pltpu.make_async_copy(v_buf.at[part], vo_hbm.at[part], vo_sem.at[i]))

    load_x = pltpu.make_async_copy(x_hbm, x_buf, x_sem)
    load_x.start()
    small = [pltpu.make_async_copy(src, dst, small_sem.at[n]) for n, (src, dst) in enumerate(
        ((gain_hbm, gain_ref), (bias_hbm, bias_ref), (bqkv_hbm, bqkv_ref), (len_hbm, len_ref)))]
    for cp in small:
        cp.start()
    for c in range(ring):
        w_load(c // n_m, c % n_m, c).start()
    load_x.wait()
    for cp in small:
        cp.wait()

    @pl.loop(0, rows // LN_ROWS)
    def _(i):
        part = pl.ds(pl.multiple_of(i * LN_ROWS, LN_ROWS), LN_ROWS)
        x = x_buf[part].astype(F32)
        mean = jnp.mean(x, axis=-1, keepdims=True)
        centered = x - mean
        var = jnp.mean(centered * centered, axis=-1, keepdims=True)
        hid[part] = (centered * lax.rsqrt(var + 1e-5) * gain_ref[...] + bias_ref[...]).astype(BF16)

    @pl.loop(0, 3)
    def _(t):
        bias = bqkv_ref[t].astype(F32)
        for m in range(n_m):
            c = t * n_m + m
            slot = lax.rem(c, ring)
            w_load(t, m, slot).wait()
            w = jnp.swapaxes(w_buf[slot], 0, 1)
            for h in range(0, heads, 2):
                r = jnp.dot(hid[:, m * mc:(m + 1) * mc], jnp.concatenate([w[h], w[h + 1]], axis=1), preferred_element_type=F32)
                for u in range(2):
                    part = r[:, u * dim:(u + 1) * dim]
                    if m:
                        part = qkv[t, h + u] + part
                    if m == n_m - 1:
                        part = (part + bias[h + u:h + u + 1]).astype(BF16).astype(F32)
                    qkv[t, h + u] = part
            ahead = m + ring

            @pl.when(c + ring < total)
            def _():
                w_load(t + ahead // n_m, ahead % n_m, slot).start()

            for at_chunk, (low, high) in enumerate(CACHE_PLAN):
                @pl.when(c == at_chunk)
                def _():
                    for i in range(low * n_blk // 8, high * n_blk // 8):
                        for cp in cache_copies(i):
                            cp.start()

    slot_id = lax.broadcasted_iota(jnp.int32, (slots, dim), 0)

    @pl.loop(0, n_blk)
    def _(i):
        for cp in cache_copies(i):
            cp.wait()
        for b in range(blk):
            at = i * blk + b
            hit = (slot_id == len_ref[at] - first)[None]
            for t, buf in ((1, k_buf), (2, v_buf)):
                new = jnp.broadcast_to(qkv[t, :, pl.ds(at, 1), :], (heads, slots, dim)).astype(BF16)
                buf[at] = jnp.where(hit, new, buf[at])
        for cp in out_copies(i):
            cp.start()

    @pl.loop(0, acc0.shape[0])
    def _(i):
        def put_stat(j, m_tile, l_tile):
            st0[i, j, 0] = m_tile
            st0[i, j, 1] = l_tile

        def put_acc(j, b, value):
            acc0[i, j, b] = value

        attend_rows(places_of(rc), lambda j, b: j * (rows // 4) + i * rc + b, slots, rc, len_ref, first, qkv, k_buf, v_buf, scores, probs, put_stat, put_acc)

    @pl.loop(0, n_blk)
    def _(i):
        for cp in out_copies(i):
            cp.wait()


LN_ROWS = 64
CACHE_PLAN = ((0, 1), (1, 2), (2, 4), (4, 6), (6, 8))


def in_hbm(*arrays):
    return [pltpu.with_memory_space_constraint(a, pltpu.HBM) for a in arrays]


def front(tok_hidden, cache_len, k_cache, v_cache, ln_gain, ln_bias, w_qkv, b_qkv, mc, ring, blk, rc):
    rows, heads, slots, dim = k_cache.shape
    width = tok_hidden.shape[1]
    vmem = pl.BlockSpec(memory_space=pltpu.VMEM)
    hbm = pl.BlockSpec(memory_space=pltpu.HBM)
    dma = pltpu.SemaphoreType.DMA
    n_blk = rows // blk
    return pl.pallas_call(
        functools.partial(front_kernel, slots, mc, blk, rc),
        in_specs=[hbm] * 8,
        out_specs=[hbm, hbm, vmem, vmem, vmem, vmem, vmem],
        out_shape=[
            jax.ShapeDtypeStruct(k_cache.shape, BF16),
            jax.ShapeDtypeStruct(v_cache.shape, BF16),
            pltpu.VMEM(k_cache.shape, BF16),
            pltpu.VMEM(v_cache.shape, BF16),
            pltpu.VMEM((3, heads, rows, dim), F32),
            pltpu.VMEM((EARLY_CHUNKS, 4, rc, heads, dim), F32),
            pltpu.VMEM((EARLY_CHUNKS, 4, 2, heads, 128), F32),
        ],
        scratch_shapes=[
            pltpu.VMEM((4 * rc, heads, heads * slots), F32), pltpu.VMEM((4 * rc, heads, heads * slots), BF16),
            pltpu.SMEM((rows,), jnp.int32), pltpu.VMEM((1, width), F32), pltpu.VMEM((1, width), F32), pltpu.VMEM(b_qkv.shape, BF16),
            pltpu.VMEM((rows, width), BF16), pltpu.VMEM((rows, width), BF16),
            pltpu.VMEM((ring, mc, heads, dim), BF16),
            dma((4,)), dma, dma((ring,)), dma((n_blk,)), dma((n_blk,)), dma((n_blk,)), dma((n_blk,)),
        ],
        compiler_params=pltpu.CompilerParams(vmem_limit_bytes=34 * 2**20),
    )(*in_hbm(cache_len, tok_hidden, ln_gain.reshape(1, width), ln_bias.reshape(1, width), w_qkv, b_qkv, k_cache, v_cache))


def combine_kernel(quarter, rc, cc, len_hbm, qkv_ref, k_ref, v_ref, acc0, st0, x_hbm, w_hbm, b_hbm, y_ref, len_ref, b_tiles, b_ref,
                   acc_ref, st_ref, scores, probs, got_acc, got_st, fwd_acc, fwd_st, own_acc, own_st, far_acc, far_st, att,
                   w_buf, x_buf, mine, near, half, far_half, tot, from_y, from_c, from_yc, load_sem, len_sem, b_sem,
                   a_s, a_r, as_s, as_r, b_s, b_r, bs_s, bs_r,
                   x_s, x_r, p_s, p_r, t_s, t_r, y_s, y_r, c_s, c_r, f_s, f_r):
    heads, slots, dim = k_ref.shape[1:]
    n_row, n_col = quarter // rc, w_hbm.shape[1] // cc
    n = n_row * n_col
    r = lax.axis_index('sp')
    z = lax.axis_index('tp')
    core, chip_y = lax.rem(r, 2), r // 2
    mate = {'sp': chip_y * 2 + (1 - core)}
    across = {'sp': (1 - chip_y) * 2 + core}
    outer = (z == 0) | (z == 3)
    inward = {'tp': jnp.where(z == 0, 1, 2)}
    outward = {'tp': jnp.where(z == 1, 0, 3)}
    peer = {'tp': 3 - z}

    load_len = pltpu.make_async_copy(len_hbm, len_ref, len_sem)
    load_len.start()
    load_b = pltpu.make_async_copy(b_hbm, b_tiles, b_sem)
    load_b.start()
    load_x = pltpu.make_async_copy(x_hbm, x_buf, load_sem.at[0])
    load_x.start()
    w_loads = []
    for j in range(n_col):
        cp = pltpu.make_async_copy(w_hbm.at[:, pl.ds(j * cc, cc)], w_buf.at[:, pl.ds(j * cc, cc)], load_sem.at[1 + j])
        cp.start()
        w_loads.append(cp)

    early = acc0.shape[0]
    for i in range(early):
        for j in range(4):
            acc_ref[pl.ds(j * quarter + i * rc, rc)] = acc0[i, j]
            st_ref[i, j] = st0[i, j]
    barrier = pltpu.get_barrier_semaphore()
    pl.semaphore_signal(barrier, inc=1, device_id=mate, device_id_type=MESH)
    pl.semaphore_signal(barrier, inc=1, device_id=across, device_id_type=MESH)

    @pl.when(outer)
    def _():
        pl.semaphore_signal(barrier, inc=1, device_id=inward, device_id_type=MESH)
        pl.semaphore_wait(barrier, 3)

    @pl.when(jnp.logical_not(outer))
    def _():
        pl.semaphore_signal(barrier, inc=1, device_id=outward, device_id_type=MESH)
        pl.semaphore_signal(barrier, inc=1, device_id=peer, device_id_type=MESH)
        pl.semaphore_wait(barrier, 4)

    def remote(src, dst, s, rcv, dev):
        return pltpu.make_async_remote_copy(src_ref=src, dst_ref=dst, send_sem=s, recv_sem=rcv, device_id=dev, device_id_type=MESH)

    mate_blocks = ((1 - chip_y) * 2 + (1 - core), chip_y * 2 + (1 - core))
    my_blocks = ((1 - chip_y) * 2 + core, chip_y * 2 + core)

    def a_stat(k, i):
        return remote(st_ref.at[i, mate_blocks[k]], got_st.at[k, i], as_s.at[k, i], as_r.at[k, i], mate)

    def a_copy(k, i):
        return remote(acc_ref.at[pl.ds(mate_blocks[k] * quarter + i * rc, rc)], got_acc.at[k, pl.ds(i * rc, rc)],
                      a_s.at[k, i], a_r.at[k, i], mate)

    def send_core(i):
        for k in range(2):
            a_stat(k, i).start()
            a_copy(k, i).start()

    for i in range(early):
        send_core(i)
    load_len.wait()
    load_b.wait()
    bias = b_tiles[...].astype(F32)
    for j in range(bias.shape[0]):
        b_ref[:, j * 128:(j + 1) * 128] = bias[j:j + 1]
    lane = lax.broadcasted_iota(jnp.int32, (heads, 128), 1)

    def join(one, two):
        top = jnp.maximum(one[0], two[0])
        f_one, f_two = jnp.exp(one[0] - top), jnp.exp(two[0] - top)
        return top, one[1] * f_one + two[1] * f_two, f_one, f_two

    def b_stat(i):
        return remote(fwd_st.at[i], far_st.at[i], bs_s.at[i], bs_r.at[i], across)

    def b_copy(i):
        return remote(fwd_acc.at[pl.ds(i * rc, rc)], far_acc.at[pl.ds(i * rc, rc)], b_s.at[i], b_r.at[i], across)

    first = r * slots
    def attend(i):
        row_at = lambda j, b: j * quarter + i * rc + b

        def put_stat(j, m_tile, l_tile):
            st_ref[i, j, 0] = m_tile
            st_ref[i, j, 1] = l_tile

        def put_acc(j, b, value):
            acc_ref[row_at(j, b)] = value

        attend_rows(places_of(rc), row_at, slots, rc, len_ref, first, qkv_ref, k_ref, v_ref, scores, probs, put_stat, put_acc)
        send_core(i)

    def join_core(i):
        for k in range(2):
            a_stat(k, i).wait()
            a_copy(k, i).wait()
            top, total, f_one, f_two = join(st_ref[i, my_blocks[k]], got_st[k, i])
            for b in range(rc):
                at = i * rc + b
                value = acc_ref[my_blocks[k] * quarter + at] * f_one[:, b:b + 1] + got_acc[k, at] * f_two[:, b:b + 1]
                if k == 0:
                    fwd_acc[at] = value
                else:
                    own_acc[at] = value
            if k == 0:
                fwd_st[i, 0] = top
                fwd_st[i, 1] = total
                b_stat(i).start()
                b_copy(i).start()
            else:
                own_st[i, 0] = top
                own_st[i, 1] = total

    def join_chips(i):
        b_stat(i).wait()
        b_copy(i).wait()
        _, total, g_one, g_two = join(own_st[i], far_st[i])
        inv = 1.0 / jnp.where(lane < rc, total, 1.0)
        g_one = g_one * inv
        g_two = g_two * inv
        for b in range(rc):
            at = i * rc + b
            own_acc[at] = own_acc[at] * g_one[:, b:b + 1] + far_acc[at] * g_two[:, b:b + 1]
        for h in range(heads):
            att[i, :, pl.ds(h * dim, dim)] = own_acc[pl.ds(i * rc, rc), h, :].astype(BF16)

    col_tile = lambda j: pl.ds(pl.multiple_of(j * cc, cc), cc)

    def finish(value, block, k):
        rows = pl.ds(pl.multiple_of(block * quarter + (k // n_col) * rc, rc), rc)
        cols = col_tile(lax.rem(k, n_col))
        y_ref[rows, cols] = (x_buf[rows, cols].astype(F32) + value + b_ref[:, cols]).astype(BF16)

    def x_copy(k):
        return remote(mine.at[k], near.at[k], x_s.at[k], x_r.at[k], inward)

    def p_copy(k):
        return remote(half.at[k], far_half.at[k], p_s.at[k], p_r.at[k], peer)

    def t_copy(k):
        return remote(tot.at[k], tot.at[k], t_s.at[k], t_r.at[k], outward)

    def y_copy(k):
        return remote(tot.at[k], from_y.at[k], y_s.at[k], y_r.at[k], across)

    def c_copy(k):
        return remote(tot.at[k], from_c.at[k], c_s.at[k], c_r.at[k], mate)

    def f_copy(k):
        return remote(from_y.at[k], from_yc.at[k], f_s.at[k], f_r.at[k], mate)

    def x_arrives(k):
        return remote(mine.at[k], near.at[k], x_s.at[k], x_r.at[k], outward)

    def t_arrives(k):
        return remote(tot.at[k], tot.at[k], t_s.at[k], t_r.at[k], inward)

    def spread(k):
        y_copy(k).start()
        c_copy(k).start()
        finish(tot[k], r, k)

    def at_lag(k, lag, do):
        if isinstance(k, int):
            if 0 <= k - lag < n:
                do(k - lag)
        else:
            pl.when((k >= lag) & (k - lag < n))(lambda: do(k - lag))

    def relay(k):
        y_copy(k).wait_recv()
        f_copy(k).start()
        finish(from_y[k], (1 - chip_y) * 2 + core, k)

    def collect(k):
        c_copy(k).wait_recv()
        finish(from_c[k], chip_y * 2 + 1 - core, k)
        f_copy(k).wait_recv()
        finish(from_yc[k], (1 - chip_y) * 2 + 1 - core, k)

    def total_inner(k):
        p_copy(k).wait_recv()
        tot[k] = half[k] + far_half[k]
        t_copy(k).start()
        spread(k)

    def total_outer(k):
        t_arrives(k).wait_recv()
        spread(k)

    def half_inner(k):
        x_arrives(k).wait_recv()
        half[k] = mine[k] + near[k]
        p_copy(k).start()

    def after(k):
        @pl.when(outer)
        def _():
            at_lag(k, LAGS_OUTER[0], total_outer)
            at_lag(k, LAGS_OUTER[1], relay)
            at_lag(k, LAGS_OUTER[2], collect)

        @pl.when(jnp.logical_not(outer))
        def _():
            at_lag(k, LAG_HALF, half_inner)
            at_lag(k, LAGS_INNER[0], total_inner)
            at_lag(k, LAGS_INNER[1], relay)
            at_lag(k, LAGS_INNER[2], collect)

    @pl.loop(0, early)
    def _(i):
        join_core(i)

    @pl.loop(early, min(early + 1, n_row))
    def _(i):
        attend(i)

    load_x.wait()
    for cp in w_loads:
        cp.wait()

    @pl.loop(early + 1, n_row)
    def _(i):
        attend(i)

    @pl.loop(early, n_row)
    def _(i):
        join_core(i)

    @pl.loop(0, n_row)
    def _(row):
        join_chips(row)

        @pl.loop(0, n_col)
        def _(j):
            k = row * n_col + j
            mine[k] = jnp.dot(att[row], w_buf[:, col_tile(j)], preferred_element_type=F32)

            @pl.when(outer)
            def _():
                x_copy(k).start()

            after(k)


    @pl.loop(n, n + max(LAGS_OUTER[2], LAGS_INNER[2]))
    def _(k):
        after(k)

    @pl.loop(0, n)
    def _(k):
        y_copy(k).wait_send()
        c_copy(k).wait_send()
        f_copy(k).wait_send()

        @pl.when(outer)
        def _():
            x_copy(k).wait_send()

        @pl.when(jnp.logical_not(outer))
        def _():
            p_copy(k).wait_send()
            t_copy(k).wait_send()


ROWS = 16
COLS = 1024
LAG_HALF = 2
EARLY_CHUNKS = 3
LAGS_INNER = (5, 8, 10)
LAGS_OUTER = (16, 20, 22)


def combine(cache_len, qkv, k_new, v_new, acc0, st0, tok_hidden, w_out, b_out, rc, cc):
    rows, heads, slots, dim = k_new.shape
    width = w_out.shape[1]
    quarter = rows // 4
    n_row, n_col = quarter // rc, width // cc
    n = n_row * n_col
    dma = pltpu.SemaphoreType.DMA
    part = pltpu.VMEM((quarter, heads, dim), F32)
    piece = pltpu.VMEM((n, rc, cc), F32)
    stat = pltpu.VMEM((n_row, 2, heads, 128), F32)
    made = [pltpu.with_memory_space_constraint(a, pltpu.VMEM) for a in (qkv, k_new, v_new, acc0, st0)]
    vmem = pl.BlockSpec(memory_space=pltpu.VMEM)
    hbm = pl.BlockSpec(memory_space=pltpu.HBM)
    return pl.pallas_call(
        functools.partial(combine_kernel, quarter, rc, cc),
        in_specs=[hbm, vmem, vmem, vmem, vmem, vmem, hbm, hbm, hbm],
        out_specs=vmem,
        out_shape=pltpu.VMEM((rows, width), BF16),
        scratch_shapes=[
            pltpu.SMEM((rows,), jnp.int32), pltpu.VMEM(b_out.shape, BF16), pltpu.VMEM((1, width), F32),
            pltpu.VMEM((rows, heads, dim), F32), pltpu.VMEM((n_row, 4, 2, heads, 128), F32),
            pltpu.VMEM((4 * rc, heads, heads * slots), F32), pltpu.VMEM((4 * rc, heads, heads * slots), BF16),
            pltpu.VMEM((2, quarter, heads, dim), F32), pltpu.VMEM((2, n_row, 2, heads, 128), F32),
            part, stat, part, stat, part, stat,
            pltpu.VMEM((n_row, rc, heads * dim), BF16),
            pltpu.VMEM(w_out.shape, BF16), pltpu.VMEM((rows, width), BF16),
            *[piece] * 8,
            dma((1 + n_col,)), dma, dma,
            *[dma((2, n_row))] * 4,
            *[dma((n_row,))] * 4,
            *[dma((n,))] * 12,
        ],
        compiler_params=pltpu.CompilerParams(collective_id=0, has_side_effects=True, vmem_limit_bytes=30 * 2**20),
    )(*in_hbm(cache_len), *made, *in_hbm(tok_hidden, w_out, b_out))


def solution(mesh):
    cache_spec = P('dp', 'tp', 'sp', None)
    row_spec = P('dp', None)

    def local_block(tok_hidden, cache_len, k_cache, v_cache, ln_gain, ln_bias, w_qkv, b_qkv, w_out, b_out):
        heads, dim, width = w_out.shape
        k_out, v_out, *parts, acc0, st0 = front(tok_hidden, cache_len, k_cache, v_cache, ln_gain, ln_bias, w_qkv, b_qkv, 2048, 3, 32, ROWS)
        k_new, v_new, qkv = parts
        y = combine(cache_len, qkv, k_new, v_new, acc0, st0, tok_hidden, w_out.reshape(heads * dim, width),
                    b_out.reshape(width // 128, 128), ROWS, COLS)
        return y, k_out, v_out

    return jax.shard_map(
        local_block,
        mesh=mesh,
        in_specs=(row_spec, P('dp'), cache_spec, cache_spec, P(None), P(None), P(None, None, 'tp', None), P(None, 'tp', None), P('tp', None, None), P(None)),
        out_specs=(row_spec, cache_spec, cache_spec),
        check_vma=False,
    )
```
